128 devices in a mesh: gx: 8 (over y, z_hi), gy: 8 (over x, core), gz: 2 (over z_lo).
Axes of the slice: x: 4, y: 4, z: 4 (z_hi: 2, z_lo: 2; z = z_hi * 2 + z_lo), core: 2. Of those that a mesh axis runs over, the one named last changes fastest.
Arguments:
- density: float32 [32, 256, 256], P('gx', 'gy', 'gz'), may hold values from 0.6 to 1.4
- velocity: float32 [3, 32, 256, 256], P(None, 'gx', 'gy', 'gz'), may hold values from -0.3 to 0.3
- solid_mask: int32 [32, 256, 256], P('gx', 'gy', 'gz'), may hold values 0 or 1
Outputs:
- density_final: float32 [32, 256, 256], P('gx', 'gy', 'gz')
- momentum: float32 [3, 32, 256, 256], P(None, 'gx', 'gy', 'gz')
The draws below stay inside these ranges and needn't reach their ends.
All inputs are finite; a program needn't handle non-finite values.
Results may differ from the reference program's by a relative error of at most 0.0003.
Values sent between devices are 32-bit elements.
No kernel may reach another device: no remote copies, remote signals or barrier semaphores. Data moves between devices by JAX's collectives and lax.ppermute only.
A program may use at most 64 MiB of HBM per device.

```python
import jax
import jax.numpy as jnp
import numpy as np
from jax import lax

ITERS = 4
NX = 32
NY = 256
NZ = 256


def set_ends(result, key, low, largest):
    shape = result.shape
    place = [jax.random.randint(jax.random.fold_in(key, axis), (), 0, shape[axis]) for axis in range(len(shape))]
    result = result.at[tuple(place)].set(low)
    longest = shape.index(max(shape))
    place[longest] = (place[longest] + 1) % shape[longest]
    return result.at[tuple(place)].set(largest)


def block_levels(stream_key, dims, cuts, low, top_value):
    gain = 1.0
    for dim, shards_of in cuts:
        steps = jax.random.uniform(jax.random.fold_in(jax.random.fold_in(stream_key, 6), dim), (shards_of,), jnp.float32, low / len(cuts), top_value / len(cuts))
        gain = gain * jnp.repeat(jnp.exp(steps), dims[dim] // shards_of).reshape((-1,) + (1,) * (len(dims) - 1 - dim))
    return gain


def centred(key, dims, spread, most, shards=(), kind=jnp.bfloat16):
    result = spread * jax.random.normal(key, dims, jnp.float32)
    if shards:
        result = result * block_levels(key, dims, shards, -0.22, 0.18)
    return jnp.clip(result, -most, most).astype(kind)


def setup_inputs(seed: int = 0) -> dict:
    arg_keys = jax.random.split(jax.random.key(seed), 4)
    return {
        "density": jnp.clip(0.6 + 0.79999995 * jax.random.uniform(arg_keys[0], (NX, NY, NZ), jnp.float32) ** block_levels(arg_keys[0], (NX, NY, NZ), ((0, 8), (1, 8), (2, 2)), -0.2, 0.2), 0.6, 1.4),
        "velocity": centred(arg_keys[1], (3, NX, NY, NZ), 0.1, 0.3, ((1, 8), (2, 8), (3, 2)), jnp.float32),
        "solid_mask": set_ends((jax.random.randint(arg_keys[2], (NX, NY, NZ), 0, 10) < 1).astype(jnp.int32), jax.random.fold_in(arg_keys[2], 1), 0, 1),
    }


VELOCITIES = [(0, 0, 0), (1, 0, 0), (-1, 0, 0), (0, 1, 0), (0, -1, 0), (0, 0, 1), (0, 0, -1),
              (1, 1, 0), (-1, -1, 0), (1, -1, 0), (-1, 1, 0), (1, 0, 1), (-1, 0, -1),
              (1, 0, -1), (-1, 0, 1), (0, 1, 1), (0, -1, -1), (0, 1, -1), (0, -1, 1)]
WEIGHTS = [1.0 / 3.0] + [1.0 / 18.0] * 6 + [1.0 / 36.0] * 12
OPPOSITE = [0, 2, 1, 4, 3, 6, 5, 8, 7, 10, 9, 12, 11, 14, 13, 16, 15, 18, 17]
RELAX_RATE = 1.25


def equilibrium(density_now, velocity_now):
    velocity_table = jnp.asarray(np.array(VELOCITIES), jnp.float32)
    projected = jnp.tensordot(velocity_table, velocity_now, axes=1, precision=lax.Precision.HIGHEST)
    speed_sq = jnp.sum(velocity_now * velocity_now, axis=0)
    weights = jnp.asarray(np.array(WEIGHTS), jnp.float32).reshape((19, 1, 1, 1))
    return weights * density_now * (1.0 + 3.0 * projected + 4.5 * projected * projected - 1.5 * speed_sq)


def moments(fields):
    velocity_table = jnp.asarray(np.array(VELOCITIES), jnp.float32)
    density_now = jnp.sum(fields, axis=0)
    momentum_now = jnp.tensordot(velocity_table.T, fields, axes=1, precision=lax.Precision.HIGHEST)
    return density_now, momentum_now


def collide(fields, solid_mask):
    density_now, momentum_now = moments(fields)
    balance = equilibrium(density_now, momentum_now / density_now)
    relaxed = fields - RELAX_RATE * (fields - balance)
    bounced = fields[np.array(OPPOSITE)]
    return jnp.where(solid_mask[None] == 1, bounced, relaxed)


def reference(density, velocity, solid_mask):
    fields = equilibrium(density, velocity)
    for iteration in range(ITERS):
        collided = collide(fields, solid_mask)
        fields = jnp.stack([jnp.roll(collided[which_pop], VELOCITIES[which_pop], axis=(0, 1, 2))
                            for which_pop in range(19)])
    density_final, momentum = moments(fields)
    return density_final, momentum
```

```python
import jax
import jax.numpy as jnp
from jax import lax
from jax.experimental import pallas as pl
from jax.experimental.pallas import tpu as pltpu
from jax.sharding import PartitionSpec as P

VELOCITIES = [
    (0, 0, 0),
    (1, 0, 0),
    (-1, 0, 0),
    (0, 1, 0),
    (0, -1, 0),
    (0, 0, 1),
    (0, 0, -1),
    (1, 1, 0),
    (-1, -1, 0),
    (1, -1, 0),
    (-1, 1, 0),
    (1, 0, 1),
    (-1, 0, -1),
    (1, 0, -1),
    (-1, 0, 1),
    (0, 1, 1),
    (0, -1, -1),
    (0, 1, -1),
    (0, -1, 1),
]
PAIRS = [(q, q + 1) for q in range(1, 19, 2)]
RELAX_RATE = 1.25
AXES = ("gx", "gy", "gz")
F32 = jnp.float32
VMEM = pl.BlockSpec(memory_space=pltpu.VMEM)
ZSHIFTED = [q for q in range(19) if VELOCITIES[q][2]]
MIB = 1 << 20


def lanes():
    return lax.broadcasted_iota(jnp.int32, (8, 128), 1)


def rows():
    return lax.broadcasted_iota(jnp.int32, (8, 128), 0)


def roll(v, shift, axis):
    shift %= v.shape[axis]
    return pltpu.roll(v, shift, axis) if shift else v


def permuted(x, target):
    pairs = []
    for gx in range(8):
        for gy in range(8):
            for gz in range(2):
                tx, ty, tz = target(gx, gy, gz)
                pairs.append(((gx * 8 + gy) * 2 + gz, ((tx % 8) * 8 + ty % 8) * 2 + tz % 2))
    return lax.ppermute(x, AXES, pairs)


def pack_kernel(d_hbm, v_hbm, m_hbm, block, zcols, d, v, m, sems):
    copies = [
        pltpu.make_async_copy(src, dst, sems.at[i])
        for i, (src, dst) in enumerate(((m_hbm, m), (v_hbm, v), (d_hbm, d)))
    ]
    for copy in copies:
        copy.start()
    for copy in copies:
        copy.wait()
    lane = lanes()
    packed = [jnp.zeros((8, 128), F32) for _ in range(5)]
    for plane in range(4):
        for t in range(4):
            at = pl.ds(8 * t, 8)
            solid = m[plane, at, :] == 1
            fields = [d[plane, at, :]]
            fields += [jnp.where(solid, -v[i, plane, at, :], v[i, plane, at, :]) for i in range(3)]
            fields.append(jnp.where(solid, 1.0, 0.0).astype(F32))
            base = plane * 32 + t * 8
            inside = (lane >= base) & (lane < base + 8)
            for f in range(5):
                block[f, plane, at, :] = fields[f]
                packed[f] = jnp.where(inside, roll(fields[f], base + 4, 1), packed[f])
    for f in range(5):
        zcols[8 * f : 8 * f + 8, :] = packed[f]


def x_message_kernel(block, zrecv, plus, minus):
    for f in range(4):
        for plane in range(4):
            slab = pl.ds((f * 4 + plane) * 32, 32)
            value = block[f, plane]
            plus[slab, :] = value
            minus[slab, :] = value
    for i in range(3):
        slab = pl.ds((16 + i) * 32, 32)
        plus[slab, :] = block[4, i + 1]
        minus[slab, :] = block[4, i]
    plus[608:648, :] = zrecv[...]
    minus[608:648, :] = zrecv[...]


def source(block, low, high, f, p, row, count):
    part, plane = divmod(p, 4)
    if part == 1:
        return block[f, plane, row : row + count, :]
    message = low if part == 0 else high
    if f < 4:
        slab = f * 4 + plane
    else:
        slab = 16 + plane - (1 if part == 0 else 0)
        if slab < 16 or slab > 18:
            return jnp.zeros((count, 128), F32)
    return message[slab * 32 + row : slab * 32 + row + count, :]


def zcolumns(zrecv, low, high, f, p):
    part = p // 4
    if part == 1:
        return zrecv[8 * f : 8 * f + 8, :]
    return (low if part == 0 else high)[608 + 8 * f : 616 + 8 * f, :]


def y_message_kernel(block, zrecv, low, high, to_core, to_chip):
    first = lax.axis_index("gy") % 2 == 0
    lane = lanes()
    for f in range(5):
        for p in range(12):
            top = source(block, low, high, f, p, 28, 4)
            bottom = source(block, low, high, f, p, 0, 4)
            at = pl.ds((f * 12 + p) * 4, 4)
            to_core[at, :] = jnp.where(first, top, bottom)
            to_chip[at, :] = jnp.where(first, bottom, top)
        edge_low = jnp.zeros((8, 128), F32)
        edge_high = jnp.zeros((8, 128), F32)
        for p in range(12):
            z = zcolumns(zrecv, low, high, f, p)
            base = (p % 4) * 32
            inside = (lane >= p * 8) & (lane < p * 8 + 8)
            edge_low = jnp.where(inside, roll(z, p * 8 - base, 1), edge_low)
            edge_high = jnp.where(inside, roll(z, p * 8 - base - 24, 1), edge_high)
        edge_high = roll(edge_high, 4, 0)
        at = pl.ds(240 + f * 4, 4)
        to_core[at, :] = jnp.where(first, edge_high, edge_low)[:4]
        to_chip[at, :] = jnp.where(first, edge_low, edge_high)[:4]


def populations(weighted, base, h, rest):
    even, odd = [], []
    double = weighted + weighted
    base2 = base + base
    for q, _ in PAIRS:
        c = VELOCITIES[q]
        terms = [(h[i], c[i]) for i in range(3) if c[i]]
        k = terms[0][0]
        if len(terms) == 2:
            k = k + terms[1][0] if terms[1][1] > 0 else k - terms[1][0]
            m = weighted * k
            even.append(base + m * k)
        else:
            m = double * k
            even.append(base2 + m * k)
        odd.append(m)
    return rest * base, even, odd


def equilibrium(density, velocity):
    h = [1.5 * u for u in velocity]
    w = density * (1.0 / 36.0)
    square = h[0] * h[0] + h[1] * h[1] + h[2] * h[2]
    still, even, odd = populations(w + w, w - w * (square * (2.0 / 3.0)), h, 12.0)
    out = [still]
    for e, o in zip(even, odd):
        out += [e + o, e - o]
    return out


def momentum_of(diff):
    total = [None, None, None]
    for (q, _), d in zip(PAIRS, diff):
        for i in range(3):
            c = VELOCITIES[q][i]
            if c:
                total[i] = d if total[i] is None else total[i] + d if c > 0 else total[i] - d
    return total


def collide(f, mask):
    total = [f[a] + f[b] for a, b in PAIRS]
    diff = [f[a] - f[b] for a, b in PAIRS]
    r = f[0]
    for s in total:
        r = r + s
    j = momentum_of(diff)
    solid = mask > 0.5
    inverse = jnp.where(solid, 0.0, 1.5 / r)
    w = jnp.where(solid, 0.0, r * (RELAX_RATE / 36.0))
    h = [x * inverse for x in j]
    square = h[0] * h[0] + h[1] * h[1] + h[2] * h[2]
    still, even, odd = populations(w + w, w - w * (square * (2.0 / 3.0)), h, 12.0)
    a = jnp.where(solid, 0.5, 0.5 * (1.0 - RELAX_RATE))
    b = jnp.where(solid, -0.5, 0.5 * (1.0 - RELAX_RATE))
    out = [still + (a + a) * f[0]]
    for s, d, e, o in zip(total, diff, even, odd):
        p, m = a * s + e, b * d + o
        out += [p + m, p - m]
    return out


def column_pull(g, src, q, p):
    cx, cy, cz = VELOCITIES[q]
    v = g[src, q, p - cx]
    if cy > 0:
        v = roll(v, 1, 0)
        v = jnp.where(rows() == 0, roll(v, 8, 1), v)
    elif cy < 0:
        v = roll(v, 7, 0)
        v = jnp.where(rows() == 7, roll(v, 120, 1), v)
    return roll(v, cz, 1)


def injected(column, q, tile):
    if VELOCITIES[q][2] > 0:
        return roll(column, -(tile * 8 + 4), 1)
    return roll(column, 127 - (64 + tile * 8 + 3), 1)


def shifted(v, q, column):
    cz = VELOCITIES[q][2]
    return jnp.where(lanes() == (0 if cz > 0 else 127), column, roll(v, cz, 1))


def main_pull(g, src, columns, p, t):
    out = []
    for q in range(19):
        cx, cy, cz = VELOCITIES[q]
        v = g[src, q, p - cx, 8 + 8 * t - cy : 16 + 8 * t - cy, :]
        out.append(shifted(v, q, injected(columns[q], q, t + 1)) if cz else v)
    return out


def frame(top, bottom):
    return jnp.where(rows() < 4, top, bottom)


def frame_pull(g, src, columns, p):
    out = []
    for q in range(19):
        cx, cy, cz = VELOCITIES[q]
        v = frame(g[src, q, p - cx, 4 - cy : 12 - cy, :], g[src, q, p - cx, 36 - cy : 44 - cy, :])
        if cz:
            column = roll(columns[q], 4, 0)
            v = shifted(v, q, frame(injected(column, q, 0), injected(column, q, 5)))
        out.append(v)
    return out


def put_frame(ref, index, v):
    ref[index + (slice(4, 8), slice(None))] = v[:4]
    ref[index + (slice(40, 44), slice(None))] = v[4:]


def lattice_kernel(block, zrecv, low, high, from_core, from_chip, density, momentum, s, hs, g, hg):
    first = lax.axis_index("gy") % 2 == 0
    lane, row = lanes(), rows()
    for f in range(5):
        for p in range(12):
            for t in range(4):
                s[f, p, 8 + 8 * t : 16 + 8 * t, :] = source(block, low, high, f, p, 8 * t, 8)
            at = pl.ds((f * 12 + p) * 4, 4)
            a, b = from_core[at, :], from_chip[at, :]
            s[f, p, 4:8, :] = jnp.where(first, b, a)
            s[f, p, 40:44, :] = jnp.where(first, a, b)
        at = pl.ds(240 + f * 4, 4)
        a, b = from_core[at, :], from_chip[at, :]
        below, above = jnp.where(first, b, a), jnp.where(first, a, b)
        edge = jnp.concatenate([above, below], axis=0)
        for p in range(12):
            own = jnp.zeros((8, 128), F32)
            for tile in range(6):
                v = s[f, p, 8 * tile : 8 * tile + 8, :]
                inside = (lane >= tile * 8) & (lane < tile * 8 + 8)
                own = jnp.where(inside, roll(v, tile * 8 + 4, 1), own)
            other = roll(zcolumns(zrecv, low, high, f, p), 8 - (p % 4) * 32, 1)
            other = jnp.where(lane < 8, roll(edge, -p * 8, 1), other)
            other = jnp.where(lane >= 40, roll(edge, 40 - p * 8, 1), other)
            inner = (lane & 4) == 0
            lower = jnp.where(inner, other, own)
            upper = jnp.where(inner, own, other)
            hs[f, p] = jnp.where(lane < 64, lower, roll(upper, 64, 1))

    def start(p, carry):
        for q, v in enumerate(equilibrium(hs[0, p], [hs[i, p] for i in (1, 2, 3)])):
            hg[0, q, p] = v
        for t in range(4):
            at = slice(8 + 8 * t, 16 + 8 * t)
            out = equilibrium(s[0, p, at, :], [s[i, p, at, :] for i in (1, 2, 3)])
            for q in range(19):
                g[0, q, p, at, :] = out[q]
        parts = [frame(s[i, p, 4:12, :], s[i, p, 36:44, :]) for i in range(4)]
        for q, v in enumerate(equilibrium(parts[0], parts[1:])):
            put_frame(g, (0, q, p), v)
        return carry

    lax.fori_loop(0, 12, start, 0)

    for step in range(3):
        src, dst = step % 2, (step + 1) % 2

        def advance(p, carry):
            columns = [column_pull(hg, src, q, p) for q in range(19)]
            for q, v in enumerate(collide(columns, hs[4, p])):
                hg[dst, q, p] = v
            for t in range(4):
                at = slice(8 + 8 * t, 16 + 8 * t)
                out = collide(main_pull(g, src, columns, p, t), s[4, p, at, :])
                for q in range(19):
                    g[dst, q, p, at, :] = out[q]
            mask = frame(s[4, p, 4:12, :], s[4, p, 36:44, :])
            for q, v in enumerate(collide(frame_pull(g, src, columns, p), mask)):
                put_frame(g, (dst, q, p), v)
            return carry

        lax.fori_loop(1 + step, 11 - step, advance, 0)

    def finish(p, carry):
        columns = [column_pull(hg, 1, q, p) if q in ZSHIFTED else None for q in range(19)]
        for t in range(4):
            at = slice(8 * t, 8 * t + 8)
            f = main_pull(g, 1, columns, p, t)
            r = f[0]
            for a, b in PAIRS:
                r = r + (f[a] + f[b])
            density[p - 4, at, :] = r
            for i, v in enumerate(momentum_of([f[a] - f[b] for a, b in PAIRS])):
                momentum[i, p - 4, at, :] = v
        return carry

    lax.fori_loop(4, 8, finish, 0)


def call(kernel, out_shape, args, *, scratch=(), specs=None, limit=2 * MIB):
    return pl.pallas_call(
        kernel,
        out_shape=out_shape,
        in_specs=specs or [VMEM] * len(args),
        out_specs=jax.tree.map(lambda _: VMEM, out_shape),
        scratch_shapes=scratch,
        compiler_params=pltpu.CompilerParams(vmem_limit_bytes=limit),
    )(*args)


def local(density, velocity, solid_mask):
    hbm = pl.BlockSpec(memory_space=pltpu.HBM)
    block, zcols = call(
        pack_kernel,
        (pltpu.VMEM((5, 4, 32, 128), F32), pltpu.VMEM((40, 128), F32)),
        (density, velocity, solid_mask),
        specs=[hbm] * 3,
        scratch=[
            pltpu.VMEM((4, 32, 128), F32),
            pltpu.VMEM((3, 4, 32, 128), F32),
            pltpu.VMEM((4, 32, 128), jnp.int32),
            pltpu.SemaphoreType.DMA((3,)),
        ],
    )
    zrecv = permuted(zcols, lambda x, y, z: (x, y, 1 - z))
    plus, minus = call(x_message_kernel, (pltpu.VMEM((648, 128), F32),) * 2, (block, zrecv))
    low = permuted(plus, lambda x, y, z: (x + 1, y, z))
    high = permuted(minus, lambda x, y, z: (x - 1, y, z))
    to_core, to_chip = call(y_message_kernel, (pltpu.VMEM((264, 128), F32),) * 2, (block, zrecv, low, high))
    from_core = permuted(to_core, lambda x, y, z: (x, y ^ 1, z))
    from_chip = permuted(to_chip, lambda x, y, z: (x, y + 1 if y % 2 else y - 1, z))
    return tuple(
        call(
            lattice_kernel,
            (jax.ShapeDtypeStruct((4, 32, 128), F32), jax.ShapeDtypeStruct((3, 4, 32, 128), F32)),
            (block, zrecv, low, high, from_core, from_chip),
            scratch=[
                pltpu.VMEM((5, 12, 48, 128), F32),
                pltpu.VMEM((5, 12, 8, 128), F32),
                pltpu.VMEM((2, 19, 12, 48, 128), F32),
                pltpu.VMEM((2, 19, 12, 8, 128), F32),
            ],
            limit=20 * MIB,
        )
    )


def solution(mesh):
    placed = (P("gx", "gy", "gz"), P(None, "gx", "gy", "gz"), P("gx", "gy", "gz"))
    return jax.shard_map(
        local,
        mesh=mesh,
        in_specs=placed,
        out_specs=(P("gx", "gy", "gz"), P(None, "gx", "gy", "gz")),
        check_vma=False,
    )
```

```python
import jax
import jax.numpy as jnp
from jax import lax
from jax.experimental import pallas as pl
from jax.experimental.pallas import tpu as pltpu
from jax.sharding import PartitionSpec as P

VELOCITIES = [
    (0, 0, 0),
    (1, 0, 0),
    (-1, 0, 0),
    (0, 1, 0),
    (0, -1, 0),
    (0, 0, 1),
    (0, 0, -1),
    (1, 1, 0),
    (-1, -1, 0),
    (1, -1, 0),
    (-1, 1, 0),
    (1, 0, 1),
    (-1, 0, -1),
    (1, 0, -1),
    (-1, 0, 1),
    (0, 1, 1),
    (0, -1, -1),
    (0, 1, -1),
    (0, -1, 1),
]
PAIRS = [(q, q + 1) for q in range(1, 19, 2)]
RELAX_RATE = 1.25
AXES = ("gx", "gy", "gz")
F32 = jnp.float32
VMEM = pl.BlockSpec(memory_space=pltpu.VMEM)
ZSHIFTED = [q for q in range(19) if VELOCITIES[q][2]]
MIB = 1 << 20
PACK_LIMIT = 66_600_000
INNER_FLOPS = 100_000_000


def lanes():
    return lax.broadcasted_iota(jnp.int32, (8, 128), 1)


def rows():
    return lax.broadcasted_iota(jnp.int32, (8, 128), 0)


def roll(v, shift, axis):
    shift %= v.shape[axis]
    return pltpu.roll(v, shift, axis) if shift else v


def permuted(x, target):
    pairs = []
    for gx in range(8):
        for gy in range(8):
            for gz in range(2):
                tx, ty, tz = target(gx, gy, gz)
                pairs.append(((gx * 8 + gy) * 2 + gz, ((tx % 8) * 8 + ty % 8) * 2 + tz % 2))
    return lax.ppermute(x, AXES, pairs)


def pack_kernel(d_hbm, v_hbm, m_hbm, block, zcols, d, v, m, sems):
    copies = [
        pltpu.make_async_copy(src, dst, sems.at[i])
        for i, (src, dst) in enumerate(((m_hbm, m), (v_hbm, v), (d_hbm, d)))
    ]
    for copy in copies:
        copy.start()
    for copy in copies:
        copy.wait()
    lane = lanes()
    packed = [jnp.zeros((8, 128), F32) for _ in range(5)]
    for plane in range(4):
        for t in range(4):
            at = pl.ds(8 * t, 8)
            solid = m[plane, at, :] == 1
            fields = [d[plane, at, :]]
            fields += [jnp.where(solid, -v[i, plane, at, :], v[i, plane, at, :]) for i in range(3)]
            fields.append(jnp.where(solid, 1.0, 0.0).astype(F32))
            base = plane * 32 + t * 8
            inside = (lane >= base) & (lane < base + 8)
            for f in range(5):
                block[f, plane, at, :] = fields[f]
                packed[f] = jnp.where(inside, roll(fields[f], base + 4, 1), packed[f])
    for f in range(5):
        zcols[8 * f : 8 * f + 8, :] = packed[f]


def x_message_kernel(block, zrecv, plus, minus):
    for f in range(4):
        for plane in range(4):
            slab = pl.ds((f * 4 + plane) * 32, 32)
            value = block[f, plane]
            plus[slab, :] = value
            minus[slab, :] = value
    for i in range(3):
        slab = pl.ds((16 + i) * 32, 32)
        plus[slab, :] = block[4, i + 1]
        minus[slab, :] = block[4, i]
    plus[608:648, :] = zrecv[...]
    minus[608:648, :] = zrecv[...]


def source(block, low, high, f, p, row, count):
    part, plane = divmod(p, 4)
    if part == 1:
        return block[f, plane, row : row + count, :]
    message = low if part == 0 else high
    if f < 4:
        slab = f * 4 + plane
    else:
        slab = 16 + plane - (1 if part == 0 else 0)
        if slab < 16 or slab > 18:
            return jnp.zeros((count, 128), F32)
    return message[slab * 32 + row : slab * 32 + row + count, :]


def zcolumns(zrecv, low, high, f, p):
    part = p // 4
    if part == 1:
        return zrecv[8 * f : 8 * f + 8, :]
    return (low if part == 0 else high)[608 + 8 * f : 616 + 8 * f, :]


def y_message_kernel(block, zrecv, low, high, to_core, to_chip):
    first = lax.axis_index("gy") % 2 == 0
    lane = lanes()
    for f in range(5):
        for p in range(12):
            top = source(block, low, high, f, p, 28, 4)
            bottom = source(block, low, high, f, p, 0, 4)
            at = pl.ds((f * 12 + p) * 4, 4)
            to_core[at, :] = jnp.where(first, top, bottom)
            to_chip[at, :] = jnp.where(first, bottom, top)
        edge_low = jnp.zeros((8, 128), F32)
        edge_high = jnp.zeros((8, 128), F32)
        for p in range(12):
            z = zcolumns(zrecv, low, high, f, p)
            base = (p % 4) * 32
            inside = (lane >= p * 8) & (lane < p * 8 + 8)
            edge_low = jnp.where(inside, roll(z, p * 8 - base, 1), edge_low)
            edge_high = jnp.where(inside, roll(z, p * 8 - base - 24, 1), edge_high)
        edge_high = roll(edge_high, 4, 0)
        at = pl.ds(240 + f * 4, 4)
        to_core[at, :] = jnp.where(first, edge_high, edge_low)[:4]
        to_chip[at, :] = jnp.where(first, edge_low, edge_high)[:4]


def populations(weighted, base, h, rest):
    even, odd = [], []
    double = weighted + weighted
    base2 = base + base
    for q, _ in PAIRS:
        c = VELOCITIES[q]
        terms = [(h[i], c[i]) for i in range(3) if c[i]]
        k = terms[0][0]
        if len(terms) == 2:
            k = k + terms[1][0] if terms[1][1] > 0 else k - terms[1][0]
            m = weighted * k
            even.append(base + m * k)
        else:
            m = double * k
            even.append(base2 + m * k)
        odd.append(m)
    return rest * base, even, odd


def equilibrium(density, velocity):
    h = [1.5 * u for u in velocity]
    w = density * (1.0 / 36.0)
    square = h[0] * h[0] + h[1] * h[1] + h[2] * h[2]
    still, even, odd = populations(w + w, w - w * (square * (2.0 / 3.0)), h, 12.0)
    out = [still]
    for e, o in zip(even, odd):
        out += [e + o, e - o]
    return out


def momentum_of(diff):
    total = [None, None, None]
    for (q, _), d in zip(PAIRS, diff):
        for i in range(3):
            c = VELOCITIES[q][i]
            if c:
                total[i] = d if total[i] is None else total[i] + d if c > 0 else total[i] - d
    return total


def collide(f, mask):
    total = [f[a] + f[b] for a, b in PAIRS]
    diff = [f[a] - f[b] for a, b in PAIRS]
    r = f[0]
    for s in total:
        r = r + s
    j = momentum_of(diff)
    solid = mask > 0.5
    inverse = jnp.where(solid, 0.0, 1.5 / r)
    w = jnp.where(solid, 0.0, r * (RELAX_RATE / 36.0))
    h = [x * inverse for x in j]
    square = h[0] * h[0] + h[1] * h[1] + h[2] * h[2]
    still, even, odd = populations(w + w, w - w * (square * (2.0 / 3.0)), h, 12.0)
    a = jnp.where(solid, 0.5, 0.5 * (1.0 - RELAX_RATE))
    b = jnp.where(solid, -0.5, 0.5 * (1.0 - RELAX_RATE))
    out = [still + (a + a) * f[0]]
    for s, d, e, o in zip(total, diff, even, odd):
        p, m = a * s + e, b * d + o
        out += [p + m, p - m]
    return out


PLUS = [5, 11, 14, 15, 18]
MINUS = [6, 12, 13, 16, 17]


def columns(hg, p, wanted):
    out = {}
    for q in wanted:
        cx, cy, cz = VELOCITIES[q]
        v = hg[p - cx, q]
        if cy:
            v = roll(v, cy, 0)
            edge = 0 if cy > 0 else 7
            out[q] = jnp.where(rows() == edge, roll(v, cz + 8 * cy, 1), roll(v, cz, 1))
        else:
            out[q] = roll(v, cz, 1)
    return out


def inject(inj, p, f, tiles):
    inner = (lanes() & 7) >= 4
    for k in range(5):
        x = jnp.where(inner, f[PLUS[k]], roll(f[MINUS[k]], 64, 1))
        for tile in tiles:
            inj[p, k, 8 * tile : 8 * tile + 8, :] = roll(x, -(tile * 8 + 4), 1)


def advance_columns(src, dst, hs, inj, planes, tiles):
    for p in planes:
        f = columns(src, p, range(19) if dst is not None else ZSHIFTED)
        inject(inj, p, f, tiles)
        if dst is not None:
            for q, v in enumerate(collide([f[q] for q in range(19)], hs[p, 4])):
                dst[p, q] = v


def pulled(load, edge):
    lane = lanes()
    sides = [edge(k) for k in range(5)]
    out = []
    for q in range(19):
        cz = VELOCITIES[q][2]
        v = load(q)
        if cz > 0:
            v = jnp.where(lane == 0, sides[PLUS.index(q)], roll(v, 1, 1))
        elif cz < 0:
            v = jnp.where(lane == 127, sides[MINUS.index(q)], roll(v, 127, 1))
        out.append(v)
    return out


def main_pull(g, inj, p, t):
    def load(q):
        cx, cy, _ = VELOCITIES[q]
        return g[p - cx, q, 8 + 8 * t - cy : 16 + 8 * t - cy, :]

    return pulled(load, lambda k: inj[p, k, 8 + 8 * t : 16 + 8 * t, :])


def framed(ref, index, radius, shift=0):
    top = ref[index + (slice(8 - radius - shift, 16 - radius - shift), slice(None))]
    bottom = ref[index + (slice(32 + radius - shift, 40 + radius - shift), slice(None))]
    return jnp.where(rows() < 4, top, bottom)


def put_framed(ref, index, radius, v):
    ref[index + (slice(8 - radius, 12 - radius), slice(None))] = v[:4]
    ref[index + (slice(36 + radius, 40 + radius), slice(None))] = v[4:]


def frame_pull(g, inj, p, radius):
    def load(q):
        cx, cy, _ = VELOCITIES[q]
        return framed(g, (p - cx, q), radius, cy)

    return pulled(load, lambda k: framed(inj, (p, k), radius))


def moments(f):
    r = f[0]
    for a, b in PAIRS:
        r = r + (f[a] + f[b])
    return [r] + momentum_of([f[a] - f[b] for a, b in PAIRS])


def inner_kernel(block, zrecv, low, high, s, hs, g0, g1, g2, g3, mid, ha, hb, inj):
    lane = lanes()
    tiles = range(1, 5)
    inner = (lane & 4) == 0
    for p in range(12):
        for f in range(5):
            own = jnp.zeros((8, 128), F32)
            for tile in tiles:
                v = source(block, low, high, f, p, 8 * tile - 8, 8)
                s[p, f, 8 * tile : 8 * tile + 8, :] = v
                inside = (lane >= tile * 8) & (lane < tile * 8 + 8)
                own = jnp.where(inside, roll(v, tile * 8 + 4, 1), own)
            other = roll(zcolumns(zrecv, low, high, f, p), 8 - (p % 4) * 32, 1)
            lower = jnp.where(inner, other, own)
            upper = jnp.where(inner, own, other)
            hs[p, f] = jnp.where(lane < 64, lower, roll(upper, 64, 1))

    def start(p, carry):
        for q, v in enumerate(equilibrium(hs[p, 0], [hs[p, i] for i in (1, 2, 3)])):
            ha[p, q] = v
        for t in range(4):
            at = slice(8 + 8 * t, 16 + 8 * t)
            for q, v in enumerate(equilibrium(s[p, 0, at, :], [s[p, i, at, :] for i in (1, 2, 3)])):
                g0[p, q, at, :] = v
        return carry

    lax.fori_loop(0, 12, start, 0)
    levels, columns_of = [g0, g1, g2, g3], [ha, hb, ha, hb]
    for step in range(3):
        src, dst = levels[step], levels[step + 1]
        planes = range(1 + step, 11 - step)
        advance_columns(columns_of[step], columns_of[step + 1], hs, inj, planes, tiles)

        def advance(p, carry):
            for t in range(4):
                at = slice(8 + 8 * t, 16 + 8 * t)
                for q, v in enumerate(collide(main_pull(src, inj, p, t), s[p, 4, at, :])):
                    dst[p, q, at, :] = v
            return carry

        lax.fori_loop(planes[0], planes[-1] + 1, advance, 0)
    advance_columns(hb, None, hs, inj, range(4, 8), tiles)

    def finish(p, carry):
        for t in range(4):
            for i, v in enumerate(moments(main_pull(g3, inj, p, t))):
                mid[i, p - 4, 8 * t : 8 * t + 8, :] = v
        return carry

    lax.fori_loop(4, 8, finish, 0)


def outer_kernel(
    from_core, from_chip, s_in, hs_in, g0_in, g1_in, g2_in, g3_in, mid, density, momentum, s, g0, g1, g2, g3, hs, ha, hb, inj
):
    del s_in, g0_in, g1_in, g2_in, g3_in
    first = lax.axis_index("gy") % 2 == 0
    lane = lanes()
    inner = (lane & 4) == 0
    for f in range(5):
        at = pl.ds(240 + f * 4, 4)
        a, b = from_core[at, :], from_chip[at, :]
        edge = jnp.concatenate([jnp.where(first, a, b), jnp.where(first, b, a)], axis=0)
        for p in range(12):
            at = pl.ds((f * 12 + p) * 4, 4)
            a, b = from_core[at, :], from_chip[at, :]
            above, below = jnp.where(first, a, b), jnp.where(first, b, a)
            s[p, f, 4:8, :] = below
            s[p, f, 40:44, :] = above
            v = jnp.concatenate([above, below], axis=0)
            own = jnp.where(lane < 8, roll(v, 4, 1), roll(v, 44, 1))
            other = jnp.where(lane < 8, roll(edge, -p * 8, 1), roll(edge, 40 - p * 8, 1))
            lower = jnp.where(inner, other, own)
            upper = jnp.where(inner, own, other)
            v = jnp.where(lane < 64, lower, roll(upper, 64, 1))
            slot = lane & 56
            hs[p, f] = jnp.where((slot == 0) | (slot == 40), v, hs_in[p, f])

    def start(p, carry):
        for q, v in enumerate(equilibrium(hs[p, 0], [hs[p, i] for i in (1, 2, 3)])):
            ha[p, q] = v
        parts = [framed(s, (p, i), 4) for i in range(4)]
        for q, v in enumerate(equilibrium(parts[0], parts[1:])):
            put_framed(g0, (p, q), 4, v)
        return carry

    lax.fori_loop(0, 12, start, 0)
    levels, columns_of = [g0, g1, g2, g3], [ha, hb, ha, hb]
    for step in range(3):
        src, dst = levels[step], levels[step + 1]
        radius = 3 - step
        planes = range(1 + step, 11 - step)
        advance_columns(columns_of[step], columns_of[step + 1], hs, inj, planes, (0, 1, 4, 5))

        def advance(p, carry):
            out = collide(frame_pull(src, inj, p, radius), framed(s, (p, 4), radius))
            for q, v in enumerate(out):
                put_framed(dst, (p, q), radius, v)
            return carry

        lax.fori_loop(planes[0], planes[-1] + 1, advance, 0, unroll=2)
    advance_columns(hb, None, hs, inj, range(4, 8), (1, 4))
    for p in range(4):
        out = moments(frame_pull(g3, inj, p + 4, 0))
        for i in range(4):
            ref, index = (density, (p,)) if i == 0 else (momentum, (i - 1, p))
            ref[index] = mid[i, p]
            ref[index + (slice(0, 4), slice(None))] = out[i][:4]
            ref[index + (slice(28, 32), slice(None))] = out[i][4:]


def call(kernel, out_shape, args, *, scratch=(), specs=None, limit=2 * MIB, flops=0, aliases=None):
    cost = pl.CostEstimate(flops=flops, bytes_accessed=0, transcendentals=0) if flops else None
    return pl.pallas_call(
        kernel,
        out_shape=out_shape,
        in_specs=specs or [VMEM] * len(args),
        out_specs=jax.tree.map(lambda _: VMEM, out_shape),
        scratch_shapes=scratch,
        input_output_aliases=aliases or {},
        cost_estimate=cost,
        compiler_params=pltpu.CompilerParams(vmem_limit_bytes=limit),
    )(*args)


def local(density, velocity, solid_mask):
    hbm = pl.BlockSpec(memory_space=pltpu.HBM)
    block, zcols = call(
        pack_kernel,
        (pltpu.VMEM((5, 4, 32, 128), F32), pltpu.VMEM((40, 128), F32)),
        (density, velocity, solid_mask),
        specs=[hbm] * 3,
        scratch=[
            pltpu.VMEM((4, 32, 128), F32),
            pltpu.VMEM((3, 4, 32, 128), F32),
            pltpu.VMEM((4, 32, 128), jnp.int32),
            pltpu.SemaphoreType.DMA((3,)),
        ],
        limit=PACK_LIMIT,
    )
    zrecv = permuted(zcols, lambda x, y, z: (x, y, 1 - z))
    plus, minus = call(x_message_kernel, (pltpu.VMEM((648, 128), F32),) * 2, (block, zrecv))
    low = permuted(plus, lambda x, y, z: (x + 1, y, z))
    high = permuted(minus, lambda x, y, z: (x - 1, y, z))
    to_core, to_chip = call(y_message_kernel, (pltpu.VMEM((264, 128), F32),) * 2, (block, zrecv, low, high))
    from_core = permuted(to_core, lambda x, y, z: (x, y ^ 1, z))
    from_chip = permuted(to_chip, lambda x, y, z: (x, y + 1 if y % 2 else y - 1, z))
    fields, level = pltpu.VMEM((12, 5, 48, 128), F32), pltpu.VMEM((12, 19, 48, 128), F32)
    column_fields, column_level = pltpu.VMEM((12, 5, 8, 128), F32), pltpu.VMEM((12, 19, 8, 128), F32)
    injected = pltpu.VMEM((12, 5, 48, 128), F32)
    s, hs, *levels, mid = call(
        inner_kernel,
        (fields, column_fields) + (level,) * 4 + (pltpu.VMEM((4, 4, 32, 128), F32),),
        (block, zrecv, low, high),
        scratch=[column_level, column_level, injected],
        limit=6 * MIB,
        flops=INNER_FLOPS,
    )
    return tuple(
        call(
            outer_kernel,
            (jax.ShapeDtypeStruct((4, 32, 128), F32), jax.ShapeDtypeStruct((3, 4, 32, 128), F32), fields) + (level,) * 4,
            (from_core, from_chip, s, hs, *levels, mid),
            scratch=[column_fields, column_level, column_level, injected],
            limit=6 * MIB,
            aliases={2: 2, 4: 3, 5: 4, 6: 5, 7: 6},
        )[:2]
    )


def solution(mesh):
    placed = (P("gx", "gy", "gz"), P(None, "gx", "gy", "gz"), P("gx", "gy", "gz"))
    return jax.shard_map(
        local,
        mesh=mesh,
        in_specs=placed,
        out_specs=(P("gx", "gy", "gz"), P(None, "gx", "gy", "gz")),
        check_vma=False,
    )
```

```python
import jax
import jax.numpy as jnp
from jax import lax
from jax.experimental import pallas as pl
from jax.experimental.pallas import tpu as pltpu
from jax.sharding import PartitionSpec as P

VELOCITIES = [
    (0, 0, 0),
    (1, 0, 0),
    (-1, 0, 0),
    (0, 1, 0),
    (0, -1, 0),
    (0, 0, 1),
    (0, 0, -1),
    (1, 1, 0),
    (-1, -1, 0),
    (1, -1, 0),
    (-1, 1, 0),
    (1, 0, 1),
    (-1, 0, -1),
    (1, 0, -1),
    (-1, 0, 1),
    (0, 1, 1),
    (0, -1, -1),
    (0, 1, -1),
    (0, -1, 1),
]
PAIRS = [(q, q + 1) for q in range(1, 19, 2)]
RELAX_RATE = 1.25
AXES = ("gx", "gy", "gz")
F32 = jnp.float32
VMEM = pl.BlockSpec(memory_space=pltpu.VMEM)
ZSHIFTED = [q for q in range(19) if VELOCITIES[q][2]]
MIB = 1 << 20
PACK_LIMIT = 66_600_000
INNER_FLOPS = 100_000_000


def lanes():
    return lax.broadcasted_iota(jnp.int32, (8, 128), 1)


def rows():
    return lax.broadcasted_iota(jnp.int32, (8, 128), 0)


def roll(v, shift, axis):
    shift %= v.shape[axis]
    return pltpu.roll(v, shift, axis) if shift else v


def permuted(x, target):
    pairs = []
    for gx in range(8):
        for gy in range(8):
            for gz in range(2):
                tx, ty, tz = target(gx, gy, gz)
                pairs.append(((gx * 8 + gy) * 2 + gz, ((tx % 8) * 8 + ty % 8) * 2 + tz % 2))
    return lax.ppermute(x, AXES, pairs)


def pack_kernel(d_hbm, v_hbm, m_hbm, block, zcols, d, v, m, sems):
    copies = [
        pltpu.make_async_copy(src, dst, sems.at[i])
        for i, (src, dst) in enumerate(((m_hbm, m), (v_hbm, v), (d_hbm, d)))
    ]
    for copy in copies:
        copy.start()
    for copy in copies:
        copy.wait()
    lane = lanes()
    packed = [jnp.zeros((8, 128), F32) for _ in range(5)]
    for plane in range(4):
        for t in range(4):
            at = pl.ds(8 * t, 8)
            solid = m[plane, at, :] == 1
            fields = [d[plane, at, :]]
            fields += [jnp.where(solid, -v[i, plane, at, :], v[i, plane, at, :]) for i in range(3)]
            fields.append(jnp.where(solid, 1.0, 0.0).astype(F32))
            base = plane * 32 + t * 8
            inside = (lane >= base) & (lane < base + 8)
            for f in range(5):
                block[f, plane, at, :] = fields[f]
                packed[f] = jnp.where(inside, roll(fields[f], base + 4, 1), packed[f])
    for f in range(5):
        zcols[8 * f : 8 * f + 8, :] = packed[f]


def x_message_kernel(block, zrecv, plus, minus):
    for f in range(4):
        for plane in range(4):
            slab = pl.ds((f * 4 + plane) * 32, 32)
            value = block[f, plane]
            plus[slab, :] = value
            minus[slab, :] = value
    for i in range(3):
        slab = pl.ds((16 + i) * 32, 32)
        plus[slab, :] = block[4, i + 1]
        minus[slab, :] = block[4, i]
    plus[608:648, :] = zrecv[...]
    minus[608:648, :] = zrecv[...]


def source(block, low, high, f, p, row, count):
    part, plane = divmod(p, 4)
    if part == 1:
        return block[f, plane, row : row + count, :]
    message = low if part == 0 else high
    if f < 4:
        slab = f * 4 + plane
    else:
        slab = 16 + plane - (1 if part == 0 else 0)
        if slab < 16 or slab > 18:
            return jnp.zeros((count, 128), F32)
    return message[slab * 32 + row : slab * 32 + row + count, :]


def zcolumns(zrecv, low, high, f, p):
    part = p // 4
    if part == 1:
        return zrecv[8 * f : 8 * f + 8, :]
    return (low if part == 0 else high)[608 + 8 * f : 616 + 8 * f, :]


def y_message_kernel(block, zrecv, low, high, to_core, to_chip):
    first = lax.axis_index("gy") % 2 == 0
    lane = lanes()
    for f in range(5):
        for p in range(12):
            top = source(block, low, high, f, p, 28, 4)
            bottom = source(block, low, high, f, p, 0, 4)
            at = pl.ds((f * 12 + p) * 4, 4)
            to_core[at, :] = jnp.where(first, top, bottom)
            to_chip[at, :] = jnp.where(first, bottom, top)
        edge_low = jnp.zeros((8, 128), F32)
        edge_high = jnp.zeros((8, 128), F32)
        for p in range(12):
            z = zcolumns(zrecv, low, high, f, p)
            base = (p % 4) * 32
            inside = (lane >= p * 8) & (lane < p * 8 + 8)
            edge_low = jnp.where(inside, roll(z, p * 8 - base, 1), edge_low)
            edge_high = jnp.where(inside, roll(z, p * 8 - base - 24, 1), edge_high)
        edge_high = roll(edge_high, 4, 0)
        at = pl.ds(240 + f * 4, 4)
        to_core[at, :] = jnp.where(first, edge_high, edge_low)[:4]
        to_chip[at, :] = jnp.where(first, edge_low, edge_high)[:4]


def populations(weighted, base, h, rest):
    even, odd = [], []
    double = weighted + weighted
    base2 = base + base
    for q, _ in PAIRS:
        c = VELOCITIES[q]
        terms = [(h[i], c[i]) for i in range(3) if c[i]]
        k = terms[0][0]
        if len(terms) == 2:
            k = k + terms[1][0] if terms[1][1] > 0 else k - terms[1][0]
            m = weighted * k
            even.append(base + m * k)
        else:
            m = double * k
            even.append(base2 + m * k)
        odd.append(m)
    return rest * base, even, odd


def equilibrium(density, velocity):
    h = [1.5 * u for u in velocity]
    w = density * (1.0 / 36.0)
    square = h[0] * h[0] + h[1] * h[1] + h[2] * h[2]
    still, even, odd = populations(w + w, w - w * (square * (2.0 / 3.0)), h, 12.0)
    out = [still]
    for e, o in zip(even, odd):
        out += [e + o, e - o]
    return out


def momentum_of(diff):
    total = [None, None, None]
    for (q, _), d in zip(PAIRS, diff):
        for i in range(3):
            c = VELOCITIES[q][i]
            if c:
                total[i] = d if total[i] is None else total[i] + d if c > 0 else total[i] - d
    return total


def collide(f, mask):
    total = [f[a] + f[b] for a, b in PAIRS]
    diff = [f[a] - f[b] for a, b in PAIRS]
    r = f[0]
    for s in total:
        r = r + s
    j = momentum_of(diff)
    solid = mask > 0.5
    inverse = jnp.where(solid, 0.0, 1.5 / r)
    w = jnp.where(solid, 0.0, r * (RELAX_RATE / 36.0))
    h = [x * inverse for x in j]
    square = h[0] * h[0] + h[1] * h[1] + h[2] * h[2]
    still, even, odd = populations(w + w, w - w * (square * (2.0 / 3.0)), h, 12.0)
    a = jnp.where(solid, 0.5, 0.5 * (1.0 - RELAX_RATE))
    b = jnp.where(solid, -0.5, 0.5 * (1.0 - RELAX_RATE))
    out = [still + (a + a) * f[0]]
    for s, d, e, o in zip(total, diff, even, odd):
        p, m = a * s + e, b * d + o
        out += [p + m, p - m]
    return out


PLUS = [5, 11, 14, 15, 18]
MINUS = [6, 12, 13, 16, 17]


def streamed_column(hg, q, p, turn=0):
    cx, cy, cz = VELOCITIES[q]
    v = hg[p - cx, q]
    if not cy:
        return roll(v, cz + turn, 1)
    v = roll(v, cy, 0)
    edge = 0 if cy > 0 else 7
    return jnp.where(rows() == edge, roll(v, cz + turn + 8 * cy, 1), roll(v, cz + turn, 1))


def advance_columns(src, dst, hs, xs, inj, planes, tiles):
    inner = (lanes() & 7) >= 4
    for p in planes:
        f = [streamed_column(src, q, p) if dst is not None or q in PLUS else None for q in range(19)]
        for k in range(5):
            xs[p, k] = jnp.where(inner, f[PLUS[k]], streamed_column(src, MINUS[k], p, 64))
        if dst is not None:
            for q, v in enumerate(collide(f, hs[p, 4])):
                dst[p, q] = v
    for p in planes:
        for k in range(5):
            x = xs[p, k]
            for tile in tiles:
                inj[p, k, 8 * tile : 8 * tile + 8, :] = roll(x, -(tile * 8 + 4), 1)


def pulled(load, edge):
    lane = lanes()
    sides = [edge(k) for k in range(5)]
    out = []
    for q in range(19):
        cz = VELOCITIES[q][2]
        v = load(q)
        if cz > 0:
            v = jnp.where(lane == 0, sides[PLUS.index(q)], roll(v, 1, 1))
        elif cz < 0:
            v = jnp.where(lane == 127, sides[MINUS.index(q)], roll(v, 127, 1))
        out.append(v)
    return out


def main_pull(g, inj, p, t):
    def load(q):
        cx, cy, _ = VELOCITIES[q]
        return g[p - cx, q, 8 + 8 * t - cy : 16 + 8 * t - cy, :]

    return pulled(load, lambda k: inj[p, k, 8 + 8 * t : 16 + 8 * t, :])


def framed(ref, index, radius, shift=0):
    top = ref[index + (slice(8 - radius - shift, 16 - radius - shift), slice(None))]
    bottom = ref[index + (slice(32 + radius - shift, 40 + radius - shift), slice(None))]
    return jnp.where(rows() < 4, top, bottom)


def put_framed(ref, index, radius, v):
    ref[index + (slice(8 - radius, 12 - radius), slice(None))] = v[:4]
    ref[index + (slice(36 + radius, 40 + radius), slice(None))] = v[4:]


def frame_pull(g, inj, p, radius):
    def load(q):
        cx, cy, _ = VELOCITIES[q]
        return framed(g, (p - cx, q), radius, cy)

    return pulled(load, lambda k: framed(inj, (p, k), radius))


def moments(f):
    r = f[0]
    for a, b in PAIRS:
        r = r + (f[a] + f[b])
    return [r] + momentum_of([f[a] - f[b] for a, b in PAIRS])


def inner_kernel(block, zrecv, low, high, s, hs, g0, g1, g2, g3, mid, ha, hb, xs, inj):
    lane = lanes()
    tiles = range(1, 5)
    inner = (lane & 4) == 0
    for p in range(12):
        for f in range(5):
            own = None
            for tile in tiles:
                v = source(block, low, high, f, p, 8 * tile - 8, 8)
                s[p, f, 8 * tile : 8 * tile + 8, :] = v
                v = roll(v, tile * 8 + 4, 1)
                own = v if own is None else jnp.where(lane >= tile * 8, v, own)
            other = roll(zcolumns(zrecv, low, high, f, p), 8 - (p % 4) * 32, 1)
            hs[p, f] = jnp.where(inner, other, own)
            xs[p, f] = jnp.where(inner, own, other)
    for p in range(12):
        for f in range(5):
            hs[p, f] = jnp.where(lane < 64, hs[p, f], roll(xs[p, f], 64, 1))

    def start(p, carry):
        for q, v in enumerate(equilibrium(hs[p, 0], [hs[p, i] for i in (1, 2, 3)])):
            ha[p, q] = v
        for t in range(4):
            at = slice(8 + 8 * t, 16 + 8 * t)
            for q, v in enumerate(equilibrium(s[p, 0, at, :], [s[p, i, at, :] for i in (1, 2, 3)])):
                g0[p, q, at, :] = v
        return carry

    lax.fori_loop(0, 12, start, 0, unroll=4)
    levels, columns_of = [g0, g1, g2, g3], [ha, hb, ha, hb]
    for step in range(3):
        src, dst = levels[step], levels[step + 1]
        planes = range(1 + step, 11 - step)
        advance_columns(columns_of[step], columns_of[step + 1], hs, xs, inj, planes, tiles)

        def advance(p, carry):
            for t in range(4):
                at = slice(8 + 8 * t, 16 + 8 * t)
                for q, v in enumerate(collide(main_pull(src, inj, p, t), s[p, 4, at, :])):
                    dst[p, q, at, :] = v
            return carry

        lax.fori_loop(planes[0], planes[-1] + 1, advance, 0, unroll=True)
    advance_columns(hb, None, hs, xs, inj, range(4, 8), tiles)

    def finish(p, carry):
        for t in range(4):
            for i, v in enumerate(moments(main_pull(g3, inj, p, t))):
                mid[i, p - 4, 8 * t : 8 * t + 8, :] = v
        return carry

    lax.fori_loop(4, 8, finish, 0, unroll=True)


def outer_kernel(
    from_core, from_chip, s_in, hs_in, g0_in, g1_in, g2_in, g3_in, mid, density, momentum, s, g0, g1, g2, g3, hs, ha, hb, xs, inj
):
    del s_in, g0_in, g1_in, g2_in, g3_in
    first = lax.axis_index("gy") % 2 == 0
    lane = lanes()
    inner = (lane & 4) == 0
    for f in range(5):
        at = pl.ds(240 + f * 4, 4)
        a, b = from_core[at, :], from_chip[at, :]
        edge = jnp.concatenate([jnp.where(first, a, b), jnp.where(first, b, a)], axis=0)
        for p in range(12):
            at = pl.ds((f * 12 + p) * 4, 4)
            a, b = from_core[at, :], from_chip[at, :]
            above, below = jnp.where(first, a, b), jnp.where(first, b, a)
            s[p, f, 4:8, :] = below
            s[p, f, 40:44, :] = above
            v = jnp.concatenate([above, below], axis=0)
            own = jnp.where(lane < 8, roll(v, 4, 1), roll(v, 44, 1))
            other = jnp.where(lane < 8, roll(edge, -p * 8, 1), roll(edge, 40 - p * 8, 1))
            hs[p, f] = jnp.where(inner, other, own)
            xs[p, f] = jnp.where(inner, own, other)
    slot = lane & 56
    added = (slot == 0) | (slot == 40)
    for p in range(12):
        for f in range(5):
            v = jnp.where(lane < 64, hs[p, f], roll(xs[p, f], 64, 1))
            hs[p, f] = jnp.where(added, v, hs_in[p, f])

    def start(p, carry):
        for q, v in enumerate(equilibrium(hs[p, 0], [hs[p, i] for i in (1, 2, 3)])):
            ha[p, q] = v
        parts = [framed(s, (p, i), 4) for i in range(4)]
        for q, v in enumerate(equilibrium(parts[0], parts[1:])):
            put_framed(g0, (p, q), 4, v)
        return carry

    lax.fori_loop(0, 12, start, 0, unroll=True)
    levels, columns_of = [g0, g1, g2, g3], [ha, hb, ha, hb]
    for step in range(3):
        src, dst = levels[step], levels[step + 1]
        radius = 3 - step
        planes = range(1 + step, 11 - step)
        advance_columns(columns_of[step], columns_of[step + 1], hs, xs, inj, planes, (0, 1, 4, 5))

        def advance(p, carry):
            out = collide(frame_pull(src, inj, p, radius), framed(s, (p, 4), radius))
            for q, v in enumerate(out):
                put_framed(dst, (p, q), radius, v)
            return carry

        lax.fori_loop(planes[0], planes[-1] + 1, advance, 0, unroll=True)
    advance_columns(hb, None, hs, xs, inj, range(4, 8), (1, 4))
    for p in range(4):
        out = moments(frame_pull(g3, inj, p + 4, 0))
        for i in range(4):
            ref, index = (density, (p,)) if i == 0 else (momentum, (i - 1, p))
            ref[index] = mid[i, p]
            ref[index + (slice(0, 4), slice(None))] = out[i][:4]
            ref[index + (slice(28, 32), slice(None))] = out[i][4:]


def call(kernel, out_shape, args, *, scratch=(), specs=None, limit=2 * MIB, flops=0, aliases=None):
    cost = pl.CostEstimate(flops=flops, bytes_accessed=0, transcendentals=0) if flops else None
    return pl.pallas_call(
        kernel,
        out_shape=out_shape,
        in_specs=specs or [VMEM] * len(args),
        out_specs=jax.tree.map(lambda _: VMEM, out_shape),
        scratch_shapes=scratch,
        input_output_aliases=aliases or {},
        cost_estimate=cost,
        compiler_params=pltpu.CompilerParams(vmem_limit_bytes=limit),
    )(*args)


def local(density, velocity, solid_mask):
    hbm = pl.BlockSpec(memory_space=pltpu.HBM)
    block, zcols = call(
        pack_kernel,
        (pltpu.VMEM((5, 4, 32, 128), F32), pltpu.VMEM((40, 128), F32)),
        (density, velocity, solid_mask),
        specs=[hbm] * 3,
        scratch=[
            pltpu.VMEM((4, 32, 128), F32),
            pltpu.VMEM((3, 4, 32, 128), F32),
            pltpu.VMEM((4, 32, 128), jnp.int32),
            pltpu.SemaphoreType.DMA((3,)),
        ],
        limit=PACK_LIMIT,
    )
    zrecv = permuted(zcols, lambda x, y, z: (x, y, 1 - z))
    plus, minus = call(x_message_kernel, (pltpu.VMEM((648, 128), F32),) * 2, (block, zrecv))
    low = permuted(plus, lambda x, y, z: (x + 1, y, z))
    high = permuted(minus, lambda x, y, z: (x - 1, y, z))
    to_core, to_chip = call(y_message_kernel, (pltpu.VMEM((264, 128), F32),) * 2, (block, zrecv, low, high))
    from_core = permuted(to_core, lambda x, y, z: (x, y ^ 1, z))
    from_chip = permuted(to_chip, lambda x, y, z: (x, y + 1 if y % 2 else y - 1, z))
    fields, level = pltpu.VMEM((12, 5, 48, 128), F32), pltpu.VMEM((12, 19, 48, 128), F32)
    column_fields, column_level = pltpu.VMEM((12, 5, 8, 128), F32), pltpu.VMEM((12, 19, 8, 128), F32)
    sides = pltpu.VMEM((12, 5, 8, 128), F32)
    injected = pltpu.VMEM((12, 5, 48, 128), F32)
    s, hs, *levels, mid = call(
        inner_kernel,
        (fields, column_fields) + (level,) * 4 + (pltpu.VMEM((4, 4, 32, 128), F32),),
        (block, zrecv, low, high),
        scratch=[column_level, column_level, sides, injected],
        limit=6 * MIB,
        flops=INNER_FLOPS,
    )
    return tuple(
        call(
            outer_kernel,
            (jax.ShapeDtypeStruct((4, 32, 128), F32), jax.ShapeDtypeStruct((3, 4, 32, 128), F32), fields) + (level,) * 4,
            (from_core, from_chip, s, hs, *levels, mid),
            scratch=[column_fields, column_level, column_level, sides, injected],
            limit=6 * MIB,
            aliases={2: 2, 4: 3, 5: 4, 6: 5, 7: 6},
        )[:2]
    )


def solution(mesh):
    placed = (P("gx", "gy", "gz"), P(None, "gx", "gy", "gz"), P("gx", "gy", "gz"))
    return jax.shard_map(
        local,
        mesh=mesh,
        in_specs=placed,
        out_specs=(P("gx", "gy", "gz"), P(None, "gx", "gy", "gz")),
        check_vma=False,
    )
```

```python
import jax
import jax.numpy as jnp
from jax import lax
from jax.experimental import pallas as pl
from jax.experimental.pallas import tpu as pltpu
from jax.sharding import PartitionSpec as P

VELOCITIES = [
    (0, 0, 0),
    (1, 0, 0),
    (-1, 0, 0),
    (0, 1, 0),
    (0, -1, 0),
    (0, 0, 1),
    (0, 0, -1),
    (1, 1, 0),
    (-1, -1, 0),
    (1, -1, 0),
    (-1, 1, 0),
    (1, 0, 1),
    (-1, 0, -1),
    (1, 0, -1),
    (-1, 0, 1),
    (0, 1, 1),
    (0, -1, -1),
    (0, 1, -1),
    (0, -1, 1),
]
PAIRS = [(q, q + 1) for q in range(1, 19, 2)]
RELAX_RATE = 1.25
AXES = ("gx", "gy", "gz")
F32 = jnp.float32
VMEM = pl.BlockSpec(memory_space=pltpu.VMEM)
ZSHIFTED = [q for q in range(19) if VELOCITIES[q][2]]
MIB = 1 << 20
PACK_LIMIT = 66_600_000
INNER_FLOPS = 100_000_000


def lanes():
    return lax.broadcasted_iota(jnp.int32, (8, 128), 1)


def rows():
    return lax.broadcasted_iota(jnp.int32, (8, 128), 0)


def roll(v, shift, axis):
    shift %= v.shape[axis]
    return pltpu.roll(v, shift, axis) if shift else v


def permuted(x, target):
    pairs = []
    for gx in range(8):
        for gy in range(8):
            for gz in range(2):
                tx, ty, tz = target(gx, gy, gz)
                pairs.append(((gx * 8 + gy) * 2 + gz, ((tx % 8) * 8 + ty % 8) * 2 + tz % 2))
    return lax.ppermute(x, AXES, pairs)


def pack_kernel(d_hbm, v_hbm, m_hbm, block, rest, zcols, d, v, m, sems):
    odd = lax.axis_index("gx") % 2
    sign = (1 - 2 * odd).astype(F32)
    copies = [
        pltpu.make_async_copy(src, dst, sems.at[i])
        for i, (src, dst) in enumerate(((m_hbm, m), (v_hbm, v), (d_hbm, d)))
    ]
    for copy in copies:
        copy.start()
    for copy in copies:
        copy.wait()
    lane = lanes()
    packed = [jnp.zeros((8, 128), F32) for _ in range(5)]
    for plane in range(4):
        for t in range(4):
            at = pl.ds(8 * t, 8)
            src = plane + odd * (3 - 2 * plane)
            solid = m[src, at, :] == 1
            fields = [d[src, at, :]]
            fields += [jnp.where(solid, -v[i, src, at, :], v[i, src, at, :]) for i in range(3)]
            fields[1] = fields[1] * sign
            fields.append(jnp.where(solid, 1.0, 0.0).astype(F32))
            base = plane * 32 + t * 8
            inside = (lane >= base) & (lane < base + 8)
            for f in range(5):
                if f < 3:
                    block[f, plane, at, :] = fields[f]
                else:
                    rest[f - 3, plane, at, :] = fields[f]
                packed[f] = jnp.where(inside, roll(fields[f], base + 4, 1), packed[f])
    for f in range(5):
        zcols[8 * f : 8 * f + 8, :] = packed[f]


def second_message_kernel(rest, zrecv, out):
    for f in range(2):
        for plane in range(4):
            slab = (f * 4 + plane) * 32
            out[slab : slab + 32, :] = rest[f, plane]
    out[256:296, :] = zrecv[...]


def source(blocks, f, p, row, count):
    first, rest = blocks[(2, 0, 1)[p // 4]]
    plane = p - 4 if 4 <= p < 8 else (11 - p if p >= 8 else 3 - p)
    if f < 3:
        v = first[f, plane, row : row + count, :]
    elif 4 <= p < 8:
        v = rest[f - 3, plane, row : row + count, :]
    else:
        slab = ((f - 3) * 4 + plane) * 32
        v = rest[slab + row : slab + row + count, :]
    return -v if f == 1 and not 4 <= p < 8 else v


def zcolumns(blocks, zrecv, f, p):
    if 4 <= p < 8:
        return zrecv[8 * f : 8 * f + 8, :], (p - 4) * 32
    v = blocks[1 if p >= 8 else 2][1][256 + 8 * f : 264 + 8 * f, :]
    return (-v if f == 1 else v), ((11 - p) if p >= 8 else (3 - p)) * 32


def y_message_kernel(first_own, rest_own, zrecv, first_pair, rest_pair, first_far, rest_far, _, to_core, to_chip):
    blocks = ((first_own, rest_own), (first_pair, rest_pair), (first_far, rest_far))
    first = lax.axis_index("gy") % 2 == 0
    lane = lanes()
    for f in range(5):
        for p in range(12):
            top = source(blocks, f, p, 28, 4)
            bottom = source(blocks, f, p, 0, 4)
            at = pl.ds((f * 12 + p) * 4, 4)
            to_core[at, :] = jnp.where(first, top, bottom)
            to_chip[at, :] = jnp.where(first, bottom, top)
        edge_low = jnp.zeros((8, 128), F32)
        edge_high = jnp.zeros((8, 128), F32)
        for p in range(12):
            z, base = zcolumns(blocks, zrecv, f, p)
            inside = (lane >= p * 8) & (lane < p * 8 + 8)
            edge_low = jnp.where(inside, roll(z, p * 8 - base, 1), edge_low)
            edge_high = jnp.where(inside, roll(z, p * 8 - base - 24, 1), edge_high)
        edge_high = roll(edge_high, 4, 0)
        at = pl.ds(240 + f * 4, 4)
        to_core[at, :] = jnp.where(first, edge_high, edge_low)[:4]
        to_chip[at, :] = jnp.where(first, edge_low, edge_high)[:4]


def populations(weighted, base, h, rest):
    even, odd = [], []
    double = weighted + weighted
    base2 = base + base
    for q, _ in PAIRS:
        c = VELOCITIES[q]
        terms = [(h[i], c[i]) for i in range(3) if c[i]]
        k = terms[0][0]
        if len(terms) == 2:
            k = k + terms[1][0] if terms[1][1] > 0 else k - terms[1][0]
            m = weighted * k
            even.append(base + m * k)
        else:
            m = double * k
            even.append(base2 + m * k)
        odd.append(m)
    return rest * base, even, odd


def equilibrium(density, velocity):
    h = [1.5 * u for u in velocity]
    w = density * (1.0 / 36.0)
    square = h[0] * h[0] + h[1] * h[1] + h[2] * h[2]
    still, even, odd = populations(w + w, w - w * (square * (2.0 / 3.0)), h, 12.0)
    out = [still]
    for e, o in zip(even, odd):
        out += [e + o, e - o]
    return out


def momentum_of(diff):
    total = [None, None, None]
    for (q, _), d in zip(PAIRS, diff):
        for i in range(3):
            c = VELOCITIES[q][i]
            if c:
                total[i] = d if total[i] is None else total[i] + d if c > 0 else total[i] - d
    return total


def collide(f, mask):
    total = [f[a] + f[b] for a, b in PAIRS]
    diff = [f[a] - f[b] for a, b in PAIRS]
    r = f[0]
    for s in total:
        r = r + s
    j = momentum_of(diff)
    solid = mask > 0.5
    inverse = jnp.where(solid, 0.0, 1.5 / r)
    w = jnp.where(solid, 0.0, r * (RELAX_RATE / 36.0))
    h = [x * inverse for x in j]
    square = h[0] * h[0] + h[1] * h[1] + h[2] * h[2]
    still, even, odd = populations(w + w, w - w * (square * (2.0 / 3.0)), h, 12.0)
    a = jnp.where(solid, 0.5, 0.5 * (1.0 - RELAX_RATE))
    b = jnp.where(solid, -0.5, 0.5 * (1.0 - RELAX_RATE))
    out = [still + (a + a) * f[0]]
    for s, d, e, o in zip(total, diff, even, odd):
        p, m = a * s + e, b * d + o
        out += [p + m, p - m]
    return out


PLUS = [5, 11, 14, 15, 18]
MINUS = [6, 12, 13, 16, 17]


def streamed_column(hg, q, p, turn=0):
    cx, cy, cz = VELOCITIES[q]
    v = hg[p - cx, q]
    if not cy:
        return roll(v, cz + turn, 1)
    v = roll(v, cy, 0)
    edge = 0 if cy > 0 else 7
    return jnp.where(rows() == edge, roll(v, cz + turn + 8 * cy, 1), roll(v, cz + turn, 1))


def advance_columns(src, dst, hs, xs, inj, planes, tiles):
    inner = (lanes() & 7) >= 4
    for p in planes:
        f = [streamed_column(src, q, p) if dst is not None or q in PLUS else None for q in range(19)]
        for k in range(5):
            xs[p, k] = jnp.where(inner, f[PLUS[k]], streamed_column(src, MINUS[k], p, 64))
        if dst is not None:
            for q, v in enumerate(collide(f, hs[p, 4])):
                dst[p, q] = v
    for p in planes:
        for k in range(5):
            x = xs[p, k]
            for tile in tiles:
                inj[p, k, 8 * tile : 8 * tile + 8, :] = roll(x, -(tile * 8 + 4), 1)


def pulled(load, edge):
    lane = lanes()
    sides = [edge(k) for k in range(5)]
    out = []
    for q in range(19):
        cz = VELOCITIES[q][2]
        v = load(q)
        if cz > 0:
            v = jnp.where(lane == 0, sides[PLUS.index(q)], roll(v, 1, 1))
        elif cz < 0:
            v = jnp.where(lane == 127, sides[MINUS.index(q)], roll(v, 127, 1))
        out.append(v)
    return out


def main_pull(g, inj, p, t):
    def load(q):
        cx, cy, _ = VELOCITIES[q]
        return g[p - cx, q, 8 + 8 * t - cy : 16 + 8 * t - cy, :]

    return pulled(load, lambda k: inj[p, k, 8 + 8 * t : 16 + 8 * t, :])


def framed(ref, index, radius, shift=0):
    top = ref[index + (slice(8 - radius - shift, 16 - radius - shift), slice(None))]
    bottom = ref[index + (slice(32 + radius - shift, 40 + radius - shift), slice(None))]
    return jnp.where(rows() < 4, top, bottom)


def put_framed(ref, index, radius, v):
    ref[index + (slice(8 - radius, 12 - radius), slice(None))] = v[:4]
    ref[index + (slice(36 + radius, 40 + radius), slice(None))] = v[4:]


def frame_pull(g, inj, p, radius):
    def load(q):
        cx, cy, _ = VELOCITIES[q]
        return framed(g, (p - cx, q), radius, cy)

    return pulled(load, lambda k: framed(inj, (p, k), radius))


def moments(f):
    r = f[0]
    for a, b in PAIRS:
        r = r + (f[a] + f[b])
    return [r] + momentum_of([f[a] - f[b] for a, b in PAIRS])


def inner(blocks, zrecv, planes, s, hs, levels, columns_of, xs, inj):
    lane = lanes()
    tiles = range(1, 5)
    inside = (lane & 4) == 0
    for p in planes[0]:
        for f in range(5):
            own = None
            for tile in tiles:
                v = source(blocks, f, p, 8 * tile - 8, 8)
                s[p, f, 8 * tile : 8 * tile + 8, :] = v
                v = roll(v, tile * 8 + 4, 1)
                own = v if own is None else jnp.where(lane >= tile * 8, v, own)
            v, base = zcolumns(blocks, zrecv, f, p)
            other = roll(v, 8 - base, 1)
            hs[p, f] = jnp.where(inside, other, own)
            xs[p, f] = jnp.where(inside, own, other)
    for p in planes[0]:
        for f in range(5):
            hs[p, f] = jnp.where(lane < 64, hs[p, f], roll(xs[p, f], 64, 1))
    for p in planes[0]:
        for q, v in enumerate(equilibrium(hs[p, 0], [hs[p, i] for i in (1, 2, 3)])):
            columns_of[0][p, q] = v
        for t in range(4):
            at = slice(8 + 8 * t, 16 + 8 * t)
            for q, v in enumerate(equilibrium(s[p, 0, at, :], [s[p, i, at, :] for i in (1, 2, 3)])):
                levels[0][p, q, at, :] = v
    for step in range(3):
        src, dst = levels[step], levels[step + 1]
        advance_columns(columns_of[step], columns_of[step + 1], hs, xs, inj, planes[step + 1], tiles)
        for p in planes[step + 1]:
            for t in range(4):
                at = slice(8 + 8 * t, 16 + 8 * t)
                for q, v in enumerate(collide(main_pull(src, inj, p, t), s[p, 4, at, :])):
                    dst[p, q, at, :] = v


NEAR = [range(4, 12), range(5, 11), range(6, 10), range(7, 9)]
FAR = [range(0, 4), range(1, 5), range(2, 6), range(3, 7)]


def near_kernel(first_own, rest_own, zrecv, first_pair, rest_pair, s, hs, g0, g1, g2, g3, h0, h1, h2, h3, xs, inj):
    blocks = ((first_own, rest_own), (first_pair, rest_pair), None)
    inner(blocks, zrecv, NEAR, s, hs, (g0, g1, g2, g3), (h0, h1, h2, h3), xs, inj)


def far_kernel(first_far, rest_far, *refs):
    s, hs, g0, g1, g2, g3, h0, h1, h2, h3, mid, xs, inj = refs[10:]
    blocks = (None, None, (first_far, rest_far))
    inner(blocks, None, FAR, s, hs, (g0, g1, g2, g3), (h0, h1, h2, h3), xs, inj)
    advance_columns(h3, None, hs, xs, inj, range(4, 8), range(1, 5))
    for p in range(4, 8):
        for t in range(4):
            for i, v in enumerate(moments(main_pull(g3, inj, p, t))):
                mid[i, p - 4, 8 * t : 8 * t + 8, :] = v


def outer_kernel(
    from_core, from_chip, s_in, hs_in, g0_in, g1_in, g2_in, g3_in, mid, density, momentum, s, g0, g1, g2, g3, hs, ha, hb, xs, inj
):
    del s_in, g0_in, g1_in, g2_in, g3_in
    first = lax.axis_index("gy") % 2 == 0
    lane = lanes()
    inner = (lane & 4) == 0
    for f in range(5):
        at = pl.ds(240 + f * 4, 4)
        a, b = from_core[at, :], from_chip[at, :]
        edge = jnp.concatenate([jnp.where(first, a, b), jnp.where(first, b, a)], axis=0)
        for p in range(12):
            at = pl.ds((f * 12 + p) * 4, 4)
            a, b = from_core[at, :], from_chip[at, :]
            above, below = jnp.where(first, a, b), jnp.where(first, b, a)
            s[p, f, 4:8, :] = below
            s[p, f, 40:44, :] = above
            v = jnp.concatenate([above, below], axis=0)
            own = jnp.where(lane < 8, roll(v, 4, 1), roll(v, 44, 1))
            other = jnp.where(lane < 8, roll(edge, -p * 8, 1), roll(edge, 40 - p * 8, 1))
            hs[p, f] = jnp.where(inner, other, own)
            xs[p, f] = jnp.where(inner, own, other)
    slot = lane & 56
    added = (slot == 0) | (slot == 40)
    for p in range(12):
        for f in range(5):
            v = jnp.where(lane < 64, hs[p, f], roll(xs[p, f], 64, 1))
            hs[p, f] = jnp.where(added, v, hs_in[p, f])

    def start(p, carry):
        for q, v in enumerate(equilibrium(hs[p, 0], [hs[p, i] for i in (1, 2, 3)])):
            ha[p, q] = v
        parts = [framed(s, (p, i), 4) for i in range(4)]
        for q, v in enumerate(equilibrium(parts[0], parts[1:])):
            put_framed(g0, (p, q), 4, v)
        return carry

    lax.fori_loop(0, 12, start, 0, unroll=True)
    levels, columns_of = [g0, g1, g2, g3], [ha, hb, ha, hb]
    for step in range(3):
        src, dst = levels[step], levels[step + 1]
        radius = 3 - step
        planes = range(1 + step, 11 - step)
        advance_columns(columns_of[step], columns_of[step + 1], hs, xs, inj, planes, (0, 1, 4, 5))

        def advance(p, carry):
            out = collide(frame_pull(src, inj, p, radius), framed(s, (p, 4), radius))
            for q, v in enumerate(out):
                put_framed(dst, (p, q), radius, v)
            return carry

        lax.fori_loop(planes[0], planes[-1] + 1, advance, 0, unroll=True)
    advance_columns(hb, None, hs, xs, inj, range(4, 8), (1, 4))
    odd = lax.axis_index("gx") % 2
    sign = (1 - 2 * odd).astype(F32)
    for p in range(4):
        out = moments(frame_pull(g3, inj, p + 4, 0))
        plane = p + odd * (3 - 2 * p)
        for i in range(4):
            ref, index = (density, (plane,)) if i == 0 else (momentum, (i - 1, plane))
            scale = sign if i == 1 else 1.0
            ref[index] = mid[i, p] * scale
            ref[index + (slice(0, 4), slice(None))] = out[i][:4] * scale
            ref[index + (slice(28, 32), slice(None))] = out[i][4:] * scale


def call(kernel, out_shape, args, *, scratch=(), specs=None, limit=2 * MIB, flops=0, aliases=None):
    cost = pl.CostEstimate(flops=flops, bytes_accessed=0, transcendentals=0) if flops else None
    return pl.pallas_call(
        kernel,
        out_shape=out_shape,
        in_specs=specs or [VMEM] * len(args),
        out_specs=jax.tree.map(lambda _: VMEM, out_shape),
        scratch_shapes=scratch,
        input_output_aliases=aliases or {},
        cost_estimate=cost,
        compiler_params=pltpu.CompilerParams(vmem_limit_bytes=limit),
    )(*args)


def local(density, velocity, solid_mask):
    hbm = pl.BlockSpec(memory_space=pltpu.HBM)
    block, rest, zcols = call(
        pack_kernel,
        (pltpu.VMEM((3, 4, 32, 128), F32), pltpu.VMEM((2, 4, 32, 128), F32), pltpu.VMEM((40, 128), F32)),
        (density, velocity, solid_mask),
        specs=[hbm] * 3,
        scratch=[
            pltpu.VMEM((4, 32, 128), F32),
            pltpu.VMEM((3, 4, 32, 128), F32),
            pltpu.VMEM((4, 32, 128), jnp.int32),
            pltpu.SemaphoreType.DMA((3,)),
        ],
        limit=PACK_LIMIT,
    )

    def pair(x, y, z):
        return x ^ 1, y, z

    def relay(x, y, z):
        return (x - 2 if x % 2 else x + 2), y, z

    zrecv = permuted(zcols, lambda x, y, z: (x, y, 1 - z))
    first_pair = permuted(block, pair)
    second = call(second_message_kernel, pltpu.VMEM((296, 128), F32), (rest, zrecv))
    rest_pair = permuted(second, pair)
    first_far = permuted(first_pair, relay)
    rest_far = permuted(rest_pair, relay)
    fields, level = pltpu.VMEM((12, 5, 48, 128), F32), pltpu.VMEM((12, 19, 48, 128), F32)
    column_fields, column_level = pltpu.VMEM((12, 5, 8, 128), F32), pltpu.VMEM((12, 19, 8, 128), F32)
    sides = pltpu.VMEM((12, 5, 8, 128), F32)
    injected = pltpu.VMEM((12, 5, 48, 128), F32)
    state = (fields, column_fields) + (level,) * 4 + (column_level,) * 4
    near = call(
        near_kernel,
        state,
        (block, rest, zrecv, first_pair, rest_pair),
        scratch=[sides, injected],
        limit=4 * MIB,
        flops=INNER_FLOPS,
    )
    to_core, to_chip = call(
        y_message_kernel,
        (pltpu.VMEM((264, 128), F32),) * 2,
        (block, rest, zrecv, first_pair, rest_pair, first_far, rest_far, near[1]),
    )
    from_core = permuted(to_core, lambda x, y, z: (x, y ^ 1, z))
    from_chip = permuted(to_chip, lambda x, y, z: (x, y + 1 if y % 2 else y - 1, z))
    *far, mid = call(
        far_kernel,
        state + (pltpu.VMEM((4, 4, 32, 128), F32),),
        (first_far, rest_far, *near),
        scratch=[sides, injected],
        limit=4 * MIB,
        flops=INNER_FLOPS,
        aliases={2 + i: i for i in range(10)},
    )
    s, hs, *levels = far[:6]
    return tuple(
        call(
            outer_kernel,
            (jax.ShapeDtypeStruct((4, 32, 128), F32), jax.ShapeDtypeStruct((3, 4, 32, 128), F32), fields) + (level,) * 4,
            (from_core, from_chip, s, hs, *levels, mid),
            scratch=[column_fields, column_level, column_level, sides, injected],
            limit=6 * MIB,
            aliases={2: 2, 4: 3, 5: 4, 6: 5, 7: 6},
        )[:2]
    )


def solution(mesh):
    placed = (P("gx", "gy", "gz"), P(None, "gx", "gy", "gz"), P("gx", "gy", "gz"))
    return jax.shard_map(
        local,
        mesh=mesh,
        in_specs=placed,
        out_specs=(P("gx", "gy", "gz"), P(None, "gx", "gy", "gz")),
        check_vma=False,
    )
```

```python
import jax
import jax.numpy as jnp
from jax import lax
from jax.experimental import pallas as pl
from jax.experimental.pallas import tpu as pltpu
from jax.sharding import PartitionSpec as P


VELOCITIES = [
    (0, 0, 0),
    (1, 0, 0),
    (-1, 0, 0),
    (0, 1, 0),
    (0, -1, 0),
    (0, 0, 1),
    (0, 0, -1),
    (1, 1, 0),
    (-1, -1, 0),
    (1, -1, 0),
    (-1, 1, 0),
    (1, 0, 1),
    (-1, 0, -1),
    (1, 0, -1),
    (-1, 0, 1),
    (0, 1, 1),
    (0, -1, -1),
    (0, 1, -1),
    (0, -1, 1),
]
PAIRS = [(q, q + 1) for q in range(1, 19, 2)]
RELAX_RATE = 1.25
AXES = ("gx", "gy", "gz")
F32 = jnp.float32
VMEM = pl.BlockSpec(memory_space=pltpu.VMEM)
MIB = 1 << 20
PACK_LIMIT = 66_600_000
INNER_FLOPS = 100_000_000


def lanes():
    return lax.broadcasted_iota(jnp.int32, (8, 128), 1)


def rows():
    return lax.broadcasted_iota(jnp.int32, (8, 128), 0)


def roll(v, shift, axis):
    shift %= v.shape[axis]
    return pltpu.roll(v, shift, axis) if shift else v


def permuted(x, target):
    pairs = []
    for gx in range(8):
        for gy in range(8):
            for gz in range(2):
                tx, ty, tz = target(gx, gy, gz)
                pairs.append(((gx * 8 + gy) * 2 + gz, ((tx % 8) * 8 + ty % 8) * 2 + tz % 2))
    return lax.ppermute(x, AXES, pairs)


def pack_kernel(d_hbm, v_hbm, m_hbm, block, rest, zcols, d, v, m, sems):
    odd = lax.axis_index("gx") % 2
    sign = (1 - 2 * odd).astype(F32)
    copies = [
        pltpu.make_async_copy(src, dst, sems.at[i])
        for i, (src, dst) in enumerate(((m_hbm, m), (v_hbm, v), (d_hbm, d)))
    ]
    for copy in copies:
        copy.start()
    for copy in copies:
        copy.wait()
    lane = lanes()
    packed = [jnp.zeros((8, 128), F32) for _ in range(5)]
    for plane in range(4):
        for t in range(4):
            at = pl.ds(8 * t, 8)
            src = plane + odd * (3 - 2 * plane)
            solid = m[src, at, :] == 1
            fields = [d[src, at, :]]
            fields += [jnp.where(solid, -v[i, src, at, :], v[i, src, at, :]) for i in range(3)]
            fields[1] = fields[1] * sign
            fields.append(jnp.where(solid, 1.0, 0.0).astype(F32))
            base = plane * 32 + t * 8
            inside = (lane >= base) & (lane < base + 8)
            for f in range(5):
                if f < 3:
                    block[f, plane, at, :] = fields[f]
                else:
                    rest[f - 3, plane, at, :] = fields[f]
                packed[f] = jnp.where(inside, roll(fields[f], base + 4, 1), packed[f])
    for f in range(5):
        zcols[8 * f : 8 * f + 8, :] = packed[f]


def second_message_kernel(rest, zrecv, out):
    for f in range(2):
        for plane in range(4):
            slab = (f * 4 + plane) * 32
            out[slab : slab + 32, :] = rest[f, plane]
    out[256:296, :] = zrecv[...]


def source(blocks, f, p, row, count):
    first, rest = blocks[(2, 0, 1)[p // 4]]
    plane = p - 4 if 4 <= p < 8 else (11 - p if p >= 8 else 3 - p)
    if f < 3:
        v = first[f, plane, row : row + count, :]
    elif 4 <= p < 8:
        v = rest[f - 3, plane, row : row + count, :]
    else:
        slab = ((f - 3) * 4 + plane) * 32
        v = rest[slab + row : slab + row + count, :]
    return -v if f == 1 and not 4 <= p < 8 else v


def zcolumns(blocks, zrecv, f, p):
    if 4 <= p < 8:
        return zrecv[8 * f : 8 * f + 8, :], (p - 4) * 32
    v = blocks[1 if p >= 8 else 2][1][256 + 8 * f : 264 + 8 * f, :]
    return (-v if f == 1 else v), ((11 - p) if p >= 8 else (3 - p)) * 32


def y_message_kernel(first_own, rest_own, zrecv, first_pair, rest_pair, to_core, to_chip):
    blocks = ((first_own, rest_own), (first_pair, rest_pair), None)
    first = lax.axis_index("gy") % 2 == 0
    lane = lanes()
    for f in range(5):
        for i in range(8):
            top = source(blocks, f, i + 4, 28, 4)
            bottom = source(blocks, f, i + 4, 0, 4)
            at = pl.ds((f * 8 + i) * 4, 4)
            to_core[at, :] = jnp.where(first, top, bottom)
            to_chip[at, :] = jnp.where(first, bottom, top)
        edge_low = jnp.zeros((8, 128), F32)
        edge_high = jnp.zeros((8, 128), F32)
        for i in range(8):
            z, base = zcolumns(blocks, zrecv, f, i + 4)
            inside = (lane >= i * 8) & (lane < i * 8 + 8)
            edge_low = jnp.where(inside, roll(z, i * 8 - base, 1), edge_low)
            edge_high = jnp.where(inside, roll(z, i * 8 - base - 24, 1), edge_high)
        edge_high = roll(edge_high, 4, 0)
        at = pl.ds(160 + f * 4, 4)
        to_core[at, :] = jnp.where(first, edge_high, edge_low)[:4]
        to_chip[at, :] = jnp.where(first, edge_low, edge_high)[:4]


def y_halo(from_core, from_chip, row):
    first = lax.axis_index("gy") % 2 == 0
    a, b = from_core[row : row + 4, :], from_chip[row : row + 4, :]
    return jnp.concatenate([jnp.where(first, a, b), jnp.where(first, b, a)], axis=0)


def halo_message_kernel(from_core, from_chip, _, out):
    for f in range(5):
        for i in range(4):
            at = (f * 4 + i) * 8
            out[at : at + 8, :] = y_halo(from_core, from_chip, (f * 8 + 4 + i) * 4)
        out[160 + 8 * f : 168 + 8 * f, :] = roll(y_halo(from_core, from_chip, 160 + f * 4), -32, 1)


def populations(weighted, base, h, rest):
    even, odd = [], []
    double = weighted + weighted
    base2 = base + base
    for q, _ in PAIRS:
        c = VELOCITIES[q]
        terms = [(h[i], c[i]) for i in range(3) if c[i]]
        k = terms[0][0]
        if len(terms) == 2:
            k = k + terms[1][0] if terms[1][1] > 0 else k - terms[1][0]
            m = weighted * k
            even.append(base + m * k)
        else:
            m = double * k
            even.append(base2 + m * k)
        odd.append(m)
    return rest * base, even, odd


def equilibrium(density, velocity):
    h = [1.5 * u for u in velocity]
    w = density * (1.0 / 36.0)
    square = h[0] * h[0] + h[1] * h[1] + h[2] * h[2]
    still, even, odd = populations(w + w, w - w * (square * (2.0 / 3.0)), h, 12.0)
    out = [still]
    for e, o in zip(even, odd):
        out += [e + o, e - o]
    return out


def momentum_of(diff):
    total = [None, None, None]
    for (q, _), d in zip(PAIRS, diff):
        for i in range(3):
            c = VELOCITIES[q][i]
            if c:
                total[i] = d if total[i] is None else total[i] + d if c > 0 else total[i] - d
    return total


def collide(f, mask):
    total = [f[a] + f[b] for a, b in PAIRS]
    diff = [f[a] - f[b] for a, b in PAIRS]
    r = f[0]
    for s in total:
        r = r + s
    j = momentum_of(diff)
    solid = mask > 0.5
    inverse = jnp.where(solid, 0.0, 1.5 / r)
    w = jnp.where(solid, 0.0, r * (RELAX_RATE / 36.0))
    h = [x * inverse for x in j]
    square = h[0] * h[0] + h[1] * h[1] + h[2] * h[2]
    still, even, odd = populations(w + w, w - w * (square * (2.0 / 3.0)), h, 12.0)
    a = jnp.where(solid, 0.5, 0.5 * (1.0 - RELAX_RATE))
    b = jnp.where(solid, -0.5, 0.5 * (1.0 - RELAX_RATE))
    out = [still + (a + a) * f[0]]
    for s, d, e, o in zip(total, diff, even, odd):
        p, m = a * s + e, b * d + o
        out += [p + m, p - m]
    return out


PLUS = [5, 11, 14, 15, 18]
MINUS = [6, 12, 13, 16, 17]


def streamed_column(hg, q, p, turn=0):
    cx, cy, cz = VELOCITIES[q]
    v = hg[p - cx, q]
    if not cy:
        return roll(v, cz + turn, 1)
    v = roll(v, cy, 0)
    edge = 0 if cy > 0 else 7
    return jnp.where(rows() == edge, roll(v, cz + turn + 8 * cy, 1), roll(v, cz + turn, 1))


def advance_columns(src, dst, hs, xs, inj, planes, tiles):
    inner = (lanes() & 7) >= 4
    for p in planes:
        f = [streamed_column(src, q, p) if dst is not None or q in PLUS else None for q in range(19)]
        for k in range(5):
            xs[p, k] = jnp.where(inner, f[PLUS[k]], streamed_column(src, MINUS[k], p, 64))
        if dst is not None:
            for q, v in enumerate(collide(f, hs[p, 4])):
                dst[p, q] = v
    for p in planes:
        for k in range(5):
            x = xs[p, k]
            for tile in tiles:
                inj[p, k, 8 * tile : 8 * tile + 8, :] = roll(x, -(tile * 8 + 4), 1)


def pulled(load, edge):
    lane = lanes()
    sides = [edge(k) for k in range(5)]
    out = []
    for q in range(19):
        cz = VELOCITIES[q][2]
        v = load(q)
        if cz > 0:
            v = jnp.where(lane == 0, sides[PLUS.index(q)], roll(v, 1, 1))
        elif cz < 0:
            v = jnp.where(lane == 127, sides[MINUS.index(q)], roll(v, 127, 1))
        out.append(v)
    return out


def main_pull(g, inj, p, t):
    def load(q):
        cx, cy, _ = VELOCITIES[q]
        return g[p - cx, q, 8 + 8 * t - cy : 16 + 8 * t - cy, :]

    return pulled(load, lambda k: inj[p, k, 8 + 8 * t : 16 + 8 * t, :])


def framed(ref, index, radius, shift=0):
    top = ref[index + (slice(8 - radius - shift, 16 - radius - shift), slice(None))]
    bottom = ref[index + (slice(32 + radius - shift, 40 + radius - shift), slice(None))]
    return jnp.where(rows() < 4, top, bottom)


def put_framed(ref, index, radius, v):
    ref[index + (slice(8 - radius, 12 - radius), slice(None))] = v[:4]
    ref[index + (slice(36 + radius, 40 + radius), slice(None))] = v[4:]


def frame_pull(g, inj, p, radius):
    def load(q):
        cx, cy, _ = VELOCITIES[q]
        return framed(g, (p - cx, q), radius, cy)

    return pulled(load, lambda k: framed(inj, (p, k), radius))


def moments(f):
    r = f[0]
    for a, b in PAIRS:
        r = r + (f[a] + f[b])
    return [r] + momentum_of([f[a] - f[b] for a, b in PAIRS])


def inner(blocks, zrecv, planes, s, hs, levels, columns_of, xs, inj, halo=None):
    lane = lanes()
    tiles = range(1, 5) if halo is None else range(6)
    inside = (lane & 4) == 0
    for p in planes[0]:
        for f in range(5):
            own = None
            if halo is not None:
                near = halo[(f * 4 + p) * 8 : (f * 4 + p) * 8 + 8, :]
                s[p, f, 4:8, :] = near[4:]
                s[p, f, 40:44, :] = near[:4]
                own = roll(near, 4, 1)
            for tile in range(1, 5):
                v = source(blocks, f, p, 8 * tile - 8, 8)
                s[p, f, 8 * tile : 8 * tile + 8, :] = v
                v = roll(v, tile * 8 + 4, 1)
                own = v if own is None else jnp.where(lane >= tile * 8, v, own)
            v, base = zcolumns(blocks, zrecv, f, p)
            other = roll(v, 8 - base, 1)
            if halo is not None:
                own = jnp.where(lane >= 40, roll(near, 44, 1), own)
                edge = halo[160 + 8 * f : 168 + 8 * f, :]
                other = jnp.where(lane < 8, roll(edge, -p * 8, 1), other)
                other = jnp.where(lane >= 40, roll(edge, 40 - p * 8, 1), other)
            hs[p, f] = jnp.where(inside, other, own)
            xs[p, f] = jnp.where(inside, own, other)
    for p in planes[0]:
        for f in range(5):
            hs[p, f] = jnp.where(lane < 64, hs[p, f], roll(xs[p, f], 64, 1))
    for p in planes[0]:
        for q, v in enumerate(equilibrium(hs[p, 0], [hs[p, i] for i in (1, 2, 3)])):
            columns_of[0][p, q] = v
        for t in range(4):
            at = slice(8 + 8 * t, 16 + 8 * t)
            for q, v in enumerate(equilibrium(s[p, 0, at, :], [s[p, i, at, :] for i in (1, 2, 3)])):
                levels[0][p, q, at, :] = v
        if halo is not None:
            start_frame(s, levels[0], p)
    for step in range(3):
        src, dst = levels[step], levels[step + 1]
        advance_columns(columns_of[step], columns_of[step + 1], hs, xs, inj, planes[step + 1], tiles)
        for p in planes[step + 1]:
            for t in range(4):
                at = slice(8 + 8 * t, 16 + 8 * t)
                for q, v in enumerate(collide(main_pull(src, inj, p, t), s[p, 4, at, :])):
                    dst[p, q, at, :] = v
            if halo is not None:
                advance_frame(src, dst, s, inj, p, 4)


def start_frame(s, g, p):
    parts = [framed(s, (p, i), 4) for i in range(4)]
    for q, v in enumerate(equilibrium(parts[0], parts[1:])):
        put_framed(g, (p, q), 4, v)


def advance_frame(src, dst, s, inj, p, radius):
    for q, v in enumerate(collide(frame_pull(src, inj, p, radius), framed(s, (p, 4), radius))):
        put_framed(dst, (p, q), radius, v)


NEAR = [range(4, 12), range(5, 11), range(6, 10), range(7, 9)]
FAR = [range(0, 4), range(1, 5), range(2, 6), range(3, 7)]


def near_kernel(first_own, rest_own, zrecv, first_pair, rest_pair, s, hs, g0, g1, g2, g3, ha, hb, xs, inj):
    blocks = ((first_own, rest_own), (first_pair, rest_pair), None)
    inner(blocks, zrecv, NEAR, s, hs, (g0, g1, g2, g3), (ha, hb, ha, hb), xs, inj)


def frame_kernel(from_core, from_chip, *refs):
    s, hs, g0, g1, g2, g3, h0, h1, h2, h3, ls, xs, inj = refs[6:]
    lane = lanes()
    inside = (lane & 4) == 0
    slot = lane & 56
    added = (slot == 0) | (slot == 40)
    for f in range(5):
        edge = y_halo(from_core, from_chip, 160 + f * 4)
        for p in NEAR[0]:
            v = y_halo(from_core, from_chip, (f * 8 + p - 4) * 4)
            s[p, f, 4:8, :] = v[4:]
            s[p, f, 40:44, :] = v[:4]
            own = jnp.where(lane < 8, roll(v, 4, 1), roll(v, 44, 1))
            other = jnp.where(lane < 8, roll(edge, -(p - 4) * 8, 1), roll(edge, 40 - (p - 4) * 8, 1))
            ls[p, f] = jnp.where(inside, other, own)
            xs[p, f] = jnp.where(inside, own, other)
    for p in NEAR[0]:
        for f in range(5):
            v = jnp.where(lane < 64, ls[p, f], roll(xs[p, f], 64, 1))
            hs[p, f] = jnp.where(added, v, hs[p, f])
    for p in NEAR[0]:
        for q, v in enumerate(equilibrium(hs[p, 0], [hs[p, i] for i in (1, 2, 3)])):
            h0[p, q] = v
        start_frame(s, g0, p)
    levels, columns_of = [g0, g1, g2, g3], [h0, h1, h2, h3]
    for step in range(3):
        src, dst = levels[step], levels[step + 1]
        advance_columns(columns_of[step], columns_of[step + 1], hs, xs, inj, NEAR[step + 1], (0, 1, 4, 5))
        for p in NEAR[step + 1]:
            advance_frame(src, dst, s, inj, p, 3 - step)


def far_kernel(first_far, rest_far, halo, *refs):
    density, momentum, s, hs, g0, g1, g2, g3, h0, h1, h2, h3, xs, inj = refs[10:]
    blocks = (None, None, (first_far, rest_far))
    inner(blocks, None, FAR, s, hs, (g0, g1, g2, g3), (h0, h1, h2, h3), xs, inj, halo)
    advance_columns(h3, None, hs, xs, inj, range(4, 8), range(1, 5))
    odd = lax.axis_index("gx") % 2
    sign = (1 - 2 * odd).astype(F32)
    for p in range(4):
        plane = p + odd * (3 - 2 * p)
        for t in range(4):
            at = slice(8 * t, 8 * t + 8)
            r, *j = moments(main_pull(g3, inj, p + 4, t))
            density[plane, at, :] = r
            j[0] = j[0] * sign
            for i in range(3):
                momentum[i, plane, at, :] = j[i]


def call(kernel, out_shape, args, *, scratch=(), specs=None, limit=2 * MIB, flops=0, aliases=None):
    cost = pl.CostEstimate(flops=flops, bytes_accessed=0, transcendentals=0) if flops else None
    return pl.pallas_call(
        kernel,
        out_shape=out_shape,
        in_specs=specs or [VMEM] * len(args),
        out_specs=jax.tree.map(lambda _: VMEM, out_shape),
        scratch_shapes=scratch,
        input_output_aliases=aliases or {},
        cost_estimate=cost,
        compiler_params=pltpu.CompilerParams(vmem_limit_bytes=limit),
    )(*args)


def local(density, velocity, solid_mask):
    hbm = pl.BlockSpec(memory_space=pltpu.HBM)
    block, rest, zcols = call(
        pack_kernel,
        (pltpu.VMEM((3, 4, 32, 128), F32), pltpu.VMEM((2, 4, 32, 128), F32), pltpu.VMEM((40, 128), F32)),
        (density, velocity, solid_mask),
        specs=[hbm] * 3,
        scratch=[
            pltpu.VMEM((4, 32, 128), F32),
            pltpu.VMEM((3, 4, 32, 128), F32),
            pltpu.VMEM((4, 32, 128), jnp.int32),
            pltpu.SemaphoreType.DMA((3,)),
        ],
        limit=PACK_LIMIT,
    )

    def pair(x, y, z):
        return x ^ 1, y, z

    def relay(x, y, z):
        return (x - 2 if x % 2 else x + 2), y, z

    zrecv = permuted(zcols, lambda x, y, z: (x, y, 1 - z))
    first_pair = permuted(block, pair)
    second = call(second_message_kernel, pltpu.VMEM((296, 128), F32), (rest, zrecv))
    rest_pair = permuted(second, pair)
    first_far = permuted(first_pair, relay)
    rest_far = permuted(rest_pair, relay)
    fields, level = pltpu.VMEM((12, 5, 48, 128), F32), pltpu.VMEM((12, 19, 48, 128), F32)
    column_fields, column_level = pltpu.VMEM((12, 5, 8, 128), F32), pltpu.VMEM((12, 19, 8, 128), F32)
    injected = pltpu.VMEM((12, 5, 48, 128), F32)
    state = (fields, column_fields) + (level,) * 4
    to_core, to_chip = call(
        y_message_kernel, (pltpu.VMEM((184, 128), F32),) * 2, (block, rest, zrecv, first_pair, rest_pair)
    )
    from_core = permuted(to_core, lambda x, y, z: (x, y ^ 1, z))
    from_chip = permuted(to_chip, lambda x, y, z: (x, y + 1 if y % 2 else y - 1, z))
    near = call(
        near_kernel,
        state,
        (block, rest, zrecv, first_pair, rest_pair),
        scratch=[column_level, column_level, column_fields, injected],
        limit=6 * MIB,
        flops=INNER_FLOPS,
    )
    halo_far = permuted(call(halo_message_kernel, pltpu.VMEM((200, 128), F32), (from_core, from_chip, near[1])), relay)
    near = call(
        frame_kernel,
        state + (column_level,) * 4,
        (from_core, from_chip, *near),
        scratch=[column_fields, column_fields, injected],
        limit=4 * MIB,
        flops=INNER_FLOPS,
        aliases={2 + i: i for i in range(6)},
    )
    outs = (jax.ShapeDtypeStruct((4, 32, 128), F32), jax.ShapeDtypeStruct((3, 4, 32, 128), F32))
    return tuple(
        call(
            far_kernel,
            outs + state + (column_level,) * 4,
            (first_far, rest_far, halo_far, *near),
            scratch=[column_fields, injected],
            limit=4 * MIB,
            flops=INNER_FLOPS,
            aliases={3 + i: 2 + i for i in range(10)},
        )[:2]
    )


def solution(mesh):
    placed = (P("gx", "gy", "gz"), P(None, "gx", "gy", "gz"), P("gx", "gy", "gz"))
    return jax.shard_map(
        local,
        mesh=mesh,
        in_specs=placed,
        out_specs=(P("gx", "gy", "gz"), P(None, "gx", "gy", "gz")),
        check_vma=False,
    )
```

```python
import jax
import jax.numpy as jnp
from jax import lax
from jax.experimental import pallas as pl
from jax.experimental.pallas import tpu as pltpu
from jax.sharding import PartitionSpec as P


VELOCITIES = [
    (0, 0, 0),
    (1, 0, 0),
    (-1, 0, 0),
    (0, 1, 0),
    (0, -1, 0),
    (0, 0, 1),
    (0, 0, -1),
    (1, 1, 0),
    (-1, -1, 0),
    (1, -1, 0),
    (-1, 1, 0),
    (1, 0, 1),
    (-1, 0, -1),
    (1, 0, -1),
    (-1, 0, 1),
    (0, 1, 1),
    (0, -1, -1),
    (0, 1, -1),
    (0, -1, 1),
]
PAIRS = [(q, q + 1) for q in range(1, 19, 2)]
RELAX_RATE = 1.25
AXES = ("gx", "gy", "gz")
F32 = jnp.float32
VMEM = pl.BlockSpec(memory_space=pltpu.VMEM)
MIB = 1 << 20
PACK_LIMIT = 66_600_000
INNER_FLOPS = 100_000_000


def lanes():
    return lax.broadcasted_iota(jnp.int32, (8, 128), 1)


def rows():
    return lax.broadcasted_iota(jnp.int32, (8, 128), 0)


def roll(v, shift, axis):
    shift %= v.shape[axis]
    return pltpu.roll(v, shift, axis) if shift else v


def permuted(x, target):
    pairs = []
    for gx in range(8):
        for gy in range(8):
            for gz in range(2):
                tx, ty, tz = target(gx, gy, gz)
                pairs.append(((gx * 8 + gy) * 2 + gz, ((tx % 8) * 8 + ty % 8) * 2 + tz % 2))
    return lax.ppermute(x, AXES, pairs)


def pack_kernel(d_hbm, v_hbm, m_hbm, block, rest, zcols, d, v, m, sems):
    odd = lax.axis_index("gx") % 2
    sign = (1 - 2 * odd).astype(F32)
    copies = [
        pltpu.make_async_copy(src, dst, sems.at[i])
        for i, (src, dst) in enumerate(((m_hbm, m), (v_hbm, v), (d_hbm, d)))
    ]
    for copy in copies:
        copy.start()
    for copy in copies:
        copy.wait()
    lane = lanes()
    packed = [jnp.zeros((8, 128), F32) for _ in range(5)]
    for plane in range(4):
        for t in range(4):
            at = pl.ds(8 * t, 8)
            src = plane + odd * (3 - 2 * plane)
            solid = m[src, at, :] == 1
            fields = [d[src, at, :]]
            fields += [jnp.where(solid, -v[i, src, at, :], v[i, src, at, :]) for i in range(3)]
            fields[1] = fields[1] * sign
            fields.append(jnp.where(solid, 1.0, 0.0).astype(F32))
            base = plane * 32 + t * 8
            inside = (lane >= base) & (lane < base + 8)
            for f in range(5):
                if f < 3:
                    block[f, plane, at, :] = fields[f]
                else:
                    rest[f - 3, plane, at, :] = fields[f]
                packed[f] = jnp.where(inside, roll(fields[f], base + 4, 1), packed[f])
    for f in range(5):
        zcols[8 * f : 8 * f + 8, :] = packed[f]


def second_message_kernel(rest, zrecv, out):
    for f in range(2):
        for plane in range(4):
            slab = (f * 4 + plane) * 32
            out[slab : slab + 32, :] = rest[f, plane]
    out[256:296, :] = zrecv[...]


def source(blocks, f, p, row, count):
    first, rest = blocks[(2, 0, 1)[p // 4]]
    plane = p - 4 if 4 <= p < 8 else (11 - p if p >= 8 else 3 - p)
    if f < 3:
        v = first[f, plane, row : row + count, :]
    elif 4 <= p < 8:
        v = rest[f - 3, plane, row : row + count, :]
    else:
        slab = ((f - 3) * 4 + plane) * 32
        v = rest[slab + row : slab + row + count, :]
    return -v if f == 1 and not 4 <= p < 8 else v


def zcolumns(blocks, zrecv, f, p):
    if 4 <= p < 8:
        return zrecv[8 * f : 8 * f + 8, :], (p - 4) * 32
    v = blocks[1 if p >= 8 else 2][1][256 + 8 * f : 264 + 8 * f, :]
    return (-v if f == 1 else v), ((11 - p) if p >= 8 else (3 - p)) * 32


def y_message_kernel(first_own, rest_own, zrecv, first_pair, rest_pair, _, to_core, to_chip):
    blocks = ((first_own, rest_own), (first_pair, rest_pair), None)
    first = lax.axis_index("gy") % 2 == 0
    lane = lanes()
    for f in range(5):
        for i in range(8):
            top = source(blocks, f, i + 4, 28, 4)
            bottom = source(blocks, f, i + 4, 0, 4)
            at = pl.ds((f * 8 + i) * 4, 4)
            to_core[at, :] = jnp.where(first, top, bottom)
            to_chip[at, :] = jnp.where(first, bottom, top)
        edge_low = jnp.zeros((8, 128), F32)
        edge_high = jnp.zeros((8, 128), F32)
        for i in range(8):
            z, base = zcolumns(blocks, zrecv, f, i + 4)
            inside = (lane >= i * 8) & (lane < i * 8 + 8)
            edge_low = jnp.where(inside, roll(z, i * 8 - base, 1), edge_low)
            edge_high = jnp.where(inside, roll(z, i * 8 - base - 24, 1), edge_high)
        edge_high = roll(edge_high, 4, 0)
        at = pl.ds(160 + f * 4, 4)
        to_core[at, :] = jnp.where(first, edge_high, edge_low)[:4]
        to_chip[at, :] = jnp.where(first, edge_low, edge_high)[:4]


def y_halo(from_core, from_chip, row):
    first = lax.axis_index("gy") % 2 == 0
    a, b = from_core[row : row + 4, :], from_chip[row : row + 4, :]
    return jnp.concatenate([jnp.where(first, a, b), jnp.where(first, b, a)], axis=0)


def halo_message_kernel(from_core, from_chip, _, out):
    for f in range(5):
        for i in range(4):
            at = (f * 4 + i) * 8
            out[at : at + 8, :] = y_halo(from_core, from_chip, (f * 8 + 4 + i) * 4)
        out[160 + 8 * f : 168 + 8 * f, :] = roll(y_halo(from_core, from_chip, 160 + f * 4), -32, 1)


def populations(weighted, base, h, rest):
    even, odd = [], []
    double = weighted + weighted
    base2 = base + base
    for q, _ in PAIRS:
        c = VELOCITIES[q]
        terms = [(h[i], c[i]) for i in range(3) if c[i]]
        k = terms[0][0]
        if len(terms) == 2:
            k = k + terms[1][0] if terms[1][1] > 0 else k - terms[1][0]
            m = weighted * k
            even.append(base + m * k)
        else:
            m = double * k
            even.append(base2 + m * k)
        odd.append(m)
    return rest * base, even, odd


def equilibrium(density, velocity):
    h = [1.5 * u for u in velocity]
    w = density * (1.0 / 36.0)
    square = h[0] * h[0] + h[1] * h[1] + h[2] * h[2]
    still, even, odd = populations(w + w, w - w * (square * (2.0 / 3.0)), h, 12.0)
    out = [still]
    for e, o in zip(even, odd):
        out += [e + o, e - o]
    return out


def momentum_of(diff):
    total = [None, None, None]
    for (q, _), d in zip(PAIRS, diff):
        for i in range(3):
            c = VELOCITIES[q][i]
            if c:
                total[i] = d if total[i] is None else total[i] + d if c > 0 else total[i] - d
    return total


def collide(f, mask):
    total = [f[a] + f[b] for a, b in PAIRS]
    diff = [f[a] - f[b] for a, b in PAIRS]
    r = f[0]
    for s in total:
        r = r + s
    j = momentum_of(diff)
    solid = mask > 0.5
    inverse = jnp.where(solid, 0.0, 1.5 / r)
    w = jnp.where(solid, 0.0, r * (RELAX_RATE / 36.0))
    h = [x * inverse for x in j]
    square = h[0] * h[0] + h[1] * h[1] + h[2] * h[2]
    still, even, odd = populations(w + w, w - w * (square * (2.0 / 3.0)), h, 12.0)
    a = jnp.where(solid, 0.5, 0.5 * (1.0 - RELAX_RATE))
    b = jnp.where(solid, -0.5, 0.5 * (1.0 - RELAX_RATE))
    out = [still + (a + a) * f[0]]
    for s, d, e, o in zip(total, diff, even, odd):
        p, m = a * s + e, b * d + o
        out += [p + m, p - m]
    return out


PLUS = [5, 11, 14, 15, 18]
MINUS = [6, 12, 13, 16, 17]


def streamed_column(hg, q, p, turn=0):
    cx, cy, cz = VELOCITIES[q]
    v = hg[p - cx, q]
    if not cy:
        return roll(v, cz + turn, 1)
    v = roll(v, cy, 0)
    edge = 0 if cy > 0 else 7
    return jnp.where(rows() == edge, roll(v, cz + turn + 8 * cy, 1), roll(v, cz + turn, 1))


def advance_columns(src, dst, hs, xs, inj, planes, tiles):
    inner = (lanes() & 7) >= 4
    for p in planes:
        f = [streamed_column(src, q, p) if dst is not None or q in PLUS else None for q in range(19)]
        for k in range(5):
            xs[p, k] = jnp.where(inner, f[PLUS[k]], streamed_column(src, MINUS[k], p, 64))
        if dst is not None:
            for q, v in enumerate(collide(f, hs[p, 4])):
                dst[p, q] = v
    for p in planes:
        for k in range(5):
            x = xs[p, k]
            for tile in tiles:
                inj[p, k, 8 * tile : 8 * tile + 8, :] = roll(x, -(tile * 8 + 4), 1)


def pulled(load, edge):
    lane = lanes()
    sides = [edge(k) for k in range(5)]
    out = []
    for q in range(19):
        cz = VELOCITIES[q][2]
        v = load(q)
        if cz > 0:
            v = jnp.where(lane == 0, sides[PLUS.index(q)], roll(v, 1, 1))
        elif cz < 0:
            v = jnp.where(lane == 127, sides[MINUS.index(q)], roll(v, 127, 1))
        out.append(v)
    return out


def main_pull(g, inj, p, t):
    def load(q):
        cx, cy, _ = VELOCITIES[q]
        return g[p - cx, q, 8 + 8 * t - cy : 16 + 8 * t - cy, :]

    return pulled(load, lambda k: inj[p, k, 8 + 8 * t : 16 + 8 * t, :])


def framed(ref, index, radius, shift=0):
    top = ref[index + (slice(8 - radius - shift, 16 - radius - shift), slice(None))]
    bottom = ref[index + (slice(32 + radius - shift, 40 + radius - shift), slice(None))]
    return jnp.where(rows() < 4, top, bottom)


def put_framed(ref, index, radius, v):
    ref[index + (slice(8 - radius, 12 - radius), slice(None))] = v[:4]
    ref[index + (slice(36 + radius, 40 + radius), slice(None))] = v[4:]


def frame_pull(g, inj, p, radius):
    def load(q):
        cx, cy, _ = VELOCITIES[q]
        return framed(g, (p - cx, q), radius, cy)

    return pulled(load, lambda k: framed(inj, (p, k), radius))


def moments(f):
    r = f[0]
    for a, b in PAIRS:
        r = r + (f[a] + f[b])
    return [r] + momentum_of([f[a] - f[b] for a, b in PAIRS])


def inner(blocks, zrecv, planes, s, hs, levels, columns_of, xs, inj):
    lane = lanes()
    tiles = range(1, 5)
    inside = (lane & 4) == 0
    for p in planes[0]:
        for f in range(5):
            own = None
            for tile in tiles:
                v = source(blocks, f, p, 8 * tile - 8, 8)
                s[p, f, 8 * tile : 8 * tile + 8, :] = v
                v = roll(v, tile * 8 + 4, 1)
                own = v if own is None else jnp.where(lane >= tile * 8, v, own)
            v, base = zcolumns(blocks, zrecv, f, p)
            other = roll(v, 8 - base, 1)
            hs[p, f] = jnp.where(inside, other, own)
            xs[p, f] = jnp.where(inside, own, other)
    for p in planes[0]:
        for f in range(5):
            hs[p, f] = jnp.where(lane < 64, hs[p, f], roll(xs[p, f], 64, 1))
    for p in planes[0]:
        for q, v in enumerate(equilibrium(hs[p, 0], [hs[p, i] for i in (1, 2, 3)])):
            columns_of[0][p, q] = v
        for t in range(4):
            at = slice(8 + 8 * t, 16 + 8 * t)
            for q, v in enumerate(equilibrium(s[p, 0, at, :], [s[p, i, at, :] for i in (1, 2, 3)])):
                levels[0][p, q, at, :] = v
    for step in range(3):
        src, dst = levels[step], levels[step + 1]
        advance_columns(columns_of[step], columns_of[step + 1], hs, xs, inj, planes[step + 1], tiles)
        for p in planes[step + 1]:
            for t in range(4):
                at = slice(8 + 8 * t, 16 + 8 * t)
                for q, v in enumerate(collide(main_pull(src, inj, p, t), s[p, 4, at, :])):
                    dst[p, q, at, :] = v


def start_frame(s, g, p):
    parts = [framed(s, (p, i), 4) for i in range(4)]
    for q, v in enumerate(equilibrium(parts[0], parts[1:])):
        put_framed(g, (p, q), 4, v)


def advance_frame(src, dst, s, inj, p, radius):
    for q, v in enumerate(collide(frame_pull(src, inj, p, radius), framed(s, (p, 4), radius))):
        put_framed(dst, (p, q), radius, v)


OWN = [range(4, 8), range(5, 7), (), ()]
PAIR = [range(8, 12), range(7, 11), range(6, 10), range(7, 9)]
NEAR = [range(4, 12), range(5, 11), range(6, 10), range(7, 9)]
FAR = [range(0, 4), range(1, 5), range(2, 6), range(3, 7)]


def own_kernel(first_own, rest_own, zrecv, s, hs, g0, g1, g2, g3, h0, h1, h2, h3, xs, inj):
    inner(((first_own, rest_own), None, None), zrecv, OWN, s, hs, (g0, g1, g2, g3), (h0, h1, h2, h3), xs, inj)


def pair_kernel(first_pair, rest_pair, *refs):
    s, hs, g0, g1, g2, g3, h0, h1, h2, h3, xs, inj = refs[10:]
    inner((None, (first_pair, rest_pair), None), None, PAIR, s, hs, (g0, g1, g2, g3), (h0, h1, h2, h3), xs, inj)


def far_kernel(first_far, rest_far, *refs):
    s, hs, g0, g1, g2, g3, h0, h1, h2, h3, mid, xs, inj = refs[10:]
    inner((None, None, (first_far, rest_far)), None, FAR, s, hs, (g0, g1, g2, g3), (h0, h1, h2, h3), xs, inj)
    advance_columns(h3, None, hs, xs, inj, range(4, 8), range(1, 5))
    for p in range(4):
        for t in range(4):
            for i, v in enumerate(moments(main_pull(g3, inj, p + 4, t))):
                mid[i, p, 8 * t : 8 * t + 8, :] = v


def frames(halo, edge, planes, s, hs, levels, columns_of, ls, xs, inj):
    lane = lanes()
    inside = (lane & 4) == 0
    slot = lane & 56
    added = (slot == 0) | (slot == 40)
    for f in range(5):
        packed = edge(f)
        for p in planes[0]:
            v = halo(f, p)
            s[p, f, 4:8, :] = v[4:]
            s[p, f, 40:44, :] = v[:4]
            own = jnp.where(lane < 8, roll(v, 4, 1), roll(v, 44, 1))
            base = (p - planes[0][0]) * 8
            other = jnp.where(lane < 8, roll(packed, -base, 1), roll(packed, 40 - base, 1))
            ls[p, f] = jnp.where(inside, other, own)
            xs[p, f] = jnp.where(inside, own, other)
    for p in planes[0]:
        for f in range(5):
            v = jnp.where(lane < 64, ls[p, f], roll(xs[p, f], 64, 1))
            hs[p, f] = jnp.where(added, v, hs[p, f])
    for p in planes[0]:
        for q, v in enumerate(equilibrium(hs[p, 0], [hs[p, i] for i in (1, 2, 3)])):
            columns_of[0][p, q] = v
        start_frame(s, levels[0], p)
    for step in range(3):
        src, dst = levels[step], levels[step + 1]
        advance_columns(columns_of[step], columns_of[step + 1], hs, xs, inj, planes[step + 1], (0, 1, 4, 5))
        for p in planes[step + 1]:
            advance_frame(src, dst, s, inj, p, 3 - step)


def near_frame_kernel(from_core, from_chip, *refs):
    s, hs, g0, g1, g2, g3, h0, h1, h2, h3, ls, xs, inj = refs[10:]
    frames(
        lambda f, p: y_halo(from_core, from_chip, (f * 8 + p - 4) * 4),
        lambda f: y_halo(from_core, from_chip, 160 + f * 4),
        NEAR, s, hs, (g0, g1, g2, g3), (h0, h1, h2, h3), ls, xs, inj,
    )


def far_frame_kernel(halo, *refs):
    mid, density, momentum, s, hs, g0, g1, g2, g3, h0, h1, h2, h3, ls, xs, inj = refs[10:]
    frames(
        lambda f, p: halo[(f * 4 + p) * 8 : (f * 4 + p) * 8 + 8, :],
        lambda f: halo[160 + 8 * f : 168 + 8 * f, :],
        FAR, s, hs, (g0, g1, g2, g3), (h0, h1, h2, h3), ls, xs, inj,
    )
    advance_columns(h3, None, hs, xs, inj, range(4, 8), (1, 4))
    odd = lax.axis_index("gx") % 2
    sign = (1 - 2 * odd).astype(F32)
    for p in range(4):
        out = moments(frame_pull(g3, inj, p + 4, 0))
        plane = p + odd * (3 - 2 * p)
        for i in range(4):
            ref, index = (density, (plane,)) if i == 0 else (momentum, (i - 1, plane))
            scale = sign if i == 1 else 1.0
            ref[index] = mid[i, p] * scale
            ref[index + (slice(0, 4), slice(None))] = out[i][:4] * scale
            ref[index + (slice(28, 32), slice(None))] = out[i][4:] * scale


def call(kernel, out_shape, args, *, scratch=(), specs=None, limit=2 * MIB, flops=0, aliases=None):
    cost = pl.CostEstimate(flops=flops, bytes_accessed=0, transcendentals=0) if flops else None
    return pl.pallas_call(
        kernel,
        out_shape=out_shape,
        in_specs=specs or [VMEM] * len(args),
        out_specs=jax.tree.map(lambda _: VMEM, out_shape),
        scratch_shapes=scratch,
        input_output_aliases=aliases or {},
        cost_estimate=cost,
        compiler_params=pltpu.CompilerParams(vmem_limit_bytes=limit),
    )(*args)


def local(density, velocity, solid_mask):
    hbm = pl.BlockSpec(memory_space=pltpu.HBM)
    block, rest, zcols = call(
        pack_kernel,
        (pltpu.VMEM((3, 4, 32, 128), F32), pltpu.VMEM((2, 4, 32, 128), F32), pltpu.VMEM((40, 128), F32)),
        (density, velocity, solid_mask),
        specs=[hbm] * 3,
        scratch=[
            pltpu.VMEM((4, 32, 128), F32),
            pltpu.VMEM((3, 4, 32, 128), F32),
            pltpu.VMEM((4, 32, 128), jnp.int32),
            pltpu.SemaphoreType.DMA((3,)),
        ],
        limit=PACK_LIMIT,
    )

    def pair(x, y, z):
        return x ^ 1, y, z

    def relay(x, y, z):
        return (x - 2 if x % 2 else x + 2), y, z

    zrecv = permuted(zcols, lambda x, y, z: (x, y, 1 - z))
    first_pair = permuted(block, pair)
    second = call(second_message_kernel, pltpu.VMEM((296, 128), F32), (rest, zrecv))
    rest_pair = permuted(second, pair)
    first_far = permuted(first_pair, relay)
    rest_far = permuted(rest_pair, relay)
    fields, level = pltpu.VMEM((12, 5, 48, 128), F32), pltpu.VMEM((12, 19, 48, 128), F32)
    column_fields, column_level = pltpu.VMEM((12, 5, 8, 128), F32), pltpu.VMEM((12, 19, 8, 128), F32)
    injected = pltpu.VMEM((12, 5, 48, 128), F32)
    state = (fields, column_fields) + (level,) * 4 + (column_level,) * 4
    work = [column_fields, injected]

    def stage(kernel, args, state_in, *, extra=(), before=(), scratch=work):
        count = len(args)
        return call(
            kernel,
            tuple(before) + state + tuple(extra),
            (*args, *state_in),
            scratch=scratch,
            limit=4 * MIB,
            flops=INNER_FLOPS,
            aliases={count + i: len(before) + i for i in range(len(state))} if state_in else None,
        )

    near = stage(own_kernel, (block, rest, zrecv), ())
    to_core, to_chip = call(
        y_message_kernel, (pltpu.VMEM((184, 128), F32),) * 2, (block, rest, zrecv, first_pair, rest_pair, near[1])
    )
    from_core = permuted(to_core, lambda x, y, z: (x, y ^ 1, z))
    from_chip = permuted(to_chip, lambda x, y, z: (x, y + 1 if y % 2 else y - 1, z))
    near = stage(pair_kernel, (first_pair, rest_pair), near)
    halo_far = permuted(call(halo_message_kernel, pltpu.VMEM((200, 128), F32), (from_core, from_chip, near[1])), relay)
    near = stage(near_frame_kernel, (from_core, from_chip), near, scratch=[column_fields, *work])
    *far, mid = stage(far_kernel, (first_far, rest_far), near, extra=[pltpu.VMEM((4, 4, 32, 128), F32)])
    outs = (jax.ShapeDtypeStruct((4, 32, 128), F32), jax.ShapeDtypeStruct((3, 4, 32, 128), F32))
    return tuple(
        call(
            far_frame_kernel,
            outs + state,
            (halo_far, *far, mid),
            scratch=[column_fields, *work],
            limit=4 * MIB,
            flops=INNER_FLOPS,
            aliases={1 + i: 2 + i for i in range(10)},
        )[:2]
    )


def solution(mesh):
    placed = (P("gx", "gy", "gz"), P(None, "gx", "gy", "gz"), P("gx", "gy", "gz"))
    return jax.shard_map(
        local,
        mesh=mesh,
        in_specs=placed,
        out_specs=(P("gx", "gy", "gz"), P(None, "gx", "gy", "gz")),
        check_vma=False,
    )
```

```python
import jax
import jax.numpy as jnp
from jax import lax
from jax.experimental import pallas as pl
from jax.experimental.pallas import tpu as pltpu
from jax.sharding import PartitionSpec as P


VELOCITIES = [
    (0, 0, 0),
    (1, 0, 0),
    (-1, 0, 0),
    (0, 1, 0),
    (0, -1, 0),
    (0, 0, 1),
    (0, 0, -1),
    (1, 1, 0),
    (-1, -1, 0),
    (1, -1, 0),
    (-1, 1, 0),
    (1, 0, 1),
    (-1, 0, -1),
    (1, 0, -1),
    (-1, 0, 1),
    (0, 1, 1),
    (0, -1, -1),
    (0, 1, -1),
    (0, -1, 1),
]
PAIRS = [(q, q + 1) for q in range(1, 19, 2)]
RELAX_RATE = 1.25
AXES = ("gx", "gy", "gz")
F32 = jnp.float32
VMEM = pl.BlockSpec(memory_space=pltpu.VMEM)
MIB = 1 << 20
PACK_LIMIT = 66_600_000
INNER_FLOPS = 100_000_000


def lanes():
    return lax.broadcasted_iota(jnp.int32, (8, 128), 1)


def rows():
    return lax.broadcasted_iota(jnp.int32, (8, 128), 0)


def roll(v, shift, axis):
    shift %= v.shape[axis]
    return pltpu.roll(v, shift, axis) if shift else v


def permuted(x, target):
    pairs = []
    for gx in range(8):
        for gy in range(8):
            for gz in range(2):
                tx, ty, tz = target(gx, gy, gz)
                pairs.append(((gx * 8 + gy) * 2 + gz, ((tx % 8) * 8 + ty % 8) * 2 + tz % 2))
    return lax.ppermute(x, AXES, pairs)


def pack_kernel(d_hbm, v_hbm, m_hbm, early, late, zcols, d, v, m, sems):
    odd = lax.axis_index("gx") % 2
    sign = (1 - 2 * odd).astype(F32)
    copies = [
        pltpu.make_async_copy(src, dst, sems.at[i])
        for i, (src, dst) in enumerate(((m_hbm, m), (v_hbm, v), (d_hbm, d)))
    ]
    for copy in copies:
        copy.start()
    for copy in copies:
        copy.wait()
    lane = lanes()
    packed = [jnp.zeros((8, 128), F32) for _ in range(5)]
    for plane in range(4):
        for t in range(4):
            at = pl.ds(8 * t, 8)
            src = plane + odd * (3 - 2 * plane)
            solid = m[src, at, :] == 1
            fields = [d[src, at, :]]
            fields += [jnp.where(solid, -v[i, src, at, :], v[i, src, at, :]) for i in range(3)]
            fields[1] = fields[1] * sign
            fields.append(jnp.where(solid, 1.0, 0.0).astype(F32))
            base = plane * 32 + t * 8
            inside = (lane >= base) & (lane < base + 8)
            for f in range(5):
                (early if plane > 1 else late)[f, plane % 2, at, :] = fields[f]
                packed[f] = jnp.where(inside, roll(fields[f], base + 4, 1), packed[f])
    for f in range(5):
        zcols[8 * f : 8 * f + 8, :] = packed[f]


def relay_message_kernel(late_pair, zdiag, out):
    for f in range(5):
        for plane in range(2):
            slab = (f * 2 + plane) * 32
            out[slab : slab + 32, :] = late_pair[f, plane]
    out[320:360, :] = zdiag[...]


def source(blocks, f, p, row, count):
    early, late, _ = blocks[p // 4]
    plane = (3 - p, p - 4, 11 - p)[p // 4]
    if plane > 1:
        v = early[f, plane - 2, row : row + count, :]
    elif p >= 4:
        v = late[f, plane, row : row + count, :]
    else:
        slab = (f * 2 + plane) * 32
        v = late[slab + row : slab + row + count, :]
    return -v if f == 1 and not 4 <= p < 8 else v


def zcolumns(blocks, f, p):
    plane = (3 - p, p - 4, 11 - p)[p // 4]
    start = (320 if p < 4 else 0) + 8 * f
    v = blocks[p // 4][2][start : start + 8, :]
    return (-v if f == 1 and not 4 <= p < 8 else v), plane * 32


def y_message_kernel(early_own, late_own, zrecv, early_pair, late_pair, zdiag, _, to_core, to_chip):
    blocks = (None, (early_own, late_own, zrecv), (early_pair, late_pair, zdiag))
    first = lax.axis_index("gy") % 2 == 0
    lane = lanes()
    for f in range(5):
        for i in range(8):
            top = source(blocks, f, i + 4, 28, 4)
            bottom = source(blocks, f, i + 4, 0, 4)
            at = pl.ds((f * 8 + i) * 4, 4)
            to_core[at, :] = jnp.where(first, top, bottom)
            to_chip[at, :] = jnp.where(first, bottom, top)
        edge_low = jnp.zeros((8, 128), F32)
        edge_high = jnp.zeros((8, 128), F32)
        for i in range(8):
            z, base = zcolumns(blocks, f, i + 4)
            inside = (lane >= i * 8) & (lane < i * 8 + 8)
            edge_low = jnp.where(inside, roll(z, i * 8 - base, 1), edge_low)
            edge_high = jnp.where(inside, roll(z, i * 8 - base - 24, 1), edge_high)
        edge_high = roll(edge_high, 4, 0)
        at = pl.ds(160 + f * 4, 4)
        to_core[at, :] = jnp.where(first, edge_high, edge_low)[:4]
        to_chip[at, :] = jnp.where(first, edge_low, edge_high)[:4]


def y_halo(from_core, from_chip, row):
    first = lax.axis_index("gy") % 2 == 0
    a, b = from_core[row : row + 4, :], from_chip[row : row + 4, :]
    return jnp.concatenate([jnp.where(first, a, b), jnp.where(first, b, a)], axis=0)


def halo_message_kernel(from_core, from_chip, _, out):
    for f in range(5):
        for i in range(4):
            at = (f * 4 + i) * 8
            out[at : at + 8, :] = y_halo(from_core, from_chip, (f * 8 + 4 + i) * 4)
        out[160 + 8 * f : 168 + 8 * f, :] = roll(y_halo(from_core, from_chip, 160 + f * 4), -32, 1)


def populations(weighted, base, h, rest):
    even, odd = [], []
    double = weighted + weighted
    base2 = base + base
    for q, _ in PAIRS:
        c = VELOCITIES[q]
        terms = [(h[i], c[i]) for i in range(3) if c[i]]
        k = terms[0][0]
        if len(terms) == 2:
            k = k + terms[1][0] if terms[1][1] > 0 else k - terms[1][0]
            m = weighted * k
            even.append(base + m * k)
        else:
            m = double * k
            even.append(base2 + m * k)
        odd.append(m)
    return rest * base, even, odd


def equilibrium(density, velocity):
    h = [1.5 * u for u in velocity]
    w = density * (1.0 / 36.0)
    square = h[0] * h[0] + h[1] * h[1] + h[2] * h[2]
    still, even, odd = populations(w + w, w - w * (square * (2.0 / 3.0)), h, 12.0)
    out = [still]
    for e, o in zip(even, odd):
        out += [e + o, e - o]
    return out


def momentum_of(diff):
    total = [None, None, None]
    for (q, _), d in zip(PAIRS, diff):
        for i in range(3):
            c = VELOCITIES[q][i]
            if c:
                total[i] = d if total[i] is None else total[i] + d if c > 0 else total[i] - d
    return total


def collide(f, mask):
    total = [f[a] + f[b] for a, b in PAIRS]
    diff = [f[a] - f[b] for a, b in PAIRS]
    r = f[0]
    for s in total:
        r = r + s
    j = momentum_of(diff)
    solid = mask > 0.5
    inverse = jnp.where(solid, 0.0, 1.5 / r)
    w = jnp.where(solid, 0.0, r * (RELAX_RATE / 36.0))
    h = [x * inverse for x in j]
    square = h[0] * h[0] + h[1] * h[1] + h[2] * h[2]
    still, even, odd = populations(w + w, w - w * (square * (2.0 / 3.0)), h, 12.0)
    a = jnp.where(solid, 0.5, 0.5 * (1.0 - RELAX_RATE))
    b = jnp.where(solid, -0.5, 0.5 * (1.0 - RELAX_RATE))
    out = [still + (a + a) * f[0]]
    for s, d, e, o in zip(total, diff, even, odd):
        p, m = a * s + e, b * d + o
        out += [p + m, p - m]
    return out


PLUS = [5, 11, 14, 15, 18]
MINUS = [6, 12, 13, 16, 17]


def streamed_column(hg, q, p, turn=0):
    cx, cy, cz = VELOCITIES[q]
    v = hg[p - cx, q]
    if not cy:
        return roll(v, cz + turn, 1)
    v = roll(v, cy, 0)
    edge = 0 if cy > 0 else 7
    return jnp.where(rows() == edge, roll(v, cz + turn + 8 * cy, 1), roll(v, cz + turn, 1))


def advance_columns(src, dst, hs, xs, inj, planes, tiles):
    inner = (lanes() & 7) >= 4
    for p in planes:
        f = [streamed_column(src, q, p) if dst is not None or q in PLUS else None for q in range(19)]
        for k in range(5):
            xs[p, k] = jnp.where(inner, f[PLUS[k]], streamed_column(src, MINUS[k], p, 64))
        if dst is not None:
            for q, v in enumerate(collide(f, hs[p, 4])):
                dst[p, q] = v
    for p in planes:
        for k in range(5):
            x = xs[p, k]
            for tile in tiles:
                inj[p, k, 8 * tile : 8 * tile + 8, :] = roll(x, -(tile * 8 + 4), 1)


def pulled(load, edge):
    lane = lanes()
    sides = [edge(k) for k in range(5)]
    out = []
    for q in range(19):
        cz = VELOCITIES[q][2]
        v = load(q)
        if cz > 0:
            v = jnp.where(lane == 0, sides[PLUS.index(q)], roll(v, 1, 1))
        elif cz < 0:
            v = jnp.where(lane == 127, sides[MINUS.index(q)], roll(v, 127, 1))
        out.append(v)
    return out


def main_pull(g, inj, p, t):
    def load(q):
        cx, cy, _ = VELOCITIES[q]
        return g[p - cx, q, 8 + 8 * t - cy : 16 + 8 * t - cy, :]

    return pulled(load, lambda k: inj[p, k, 8 + 8 * t : 16 + 8 * t, :])


def framed(ref, index, radius, shift=0):
    top = ref[index + (slice(8 - radius - shift, 16 - radius - shift), slice(None))]
    bottom = ref[index + (slice(32 + radius - shift, 40 + radius - shift), slice(None))]
    return jnp.where(rows() < 4, top, bottom)


def put_framed(ref, index, radius, v):
    ref[index + (slice(8 - radius, 12 - radius), slice(None))] = v[:4]
    ref[index + (slice(36 + radius, 40 + radius), slice(None))] = v[4:]


def frame_pull(g, inj, p, radius):
    def load(q):
        cx, cy, _ = VELOCITIES[q]
        return framed(g, (p - cx, q), radius, cy)

    return pulled(load, lambda k: framed(inj, (p, k), radius))


def moments(f):
    r = f[0]
    for a, b in PAIRS:
        r = r + (f[a] + f[b])
    return [r] + momentum_of([f[a] - f[b] for a, b in PAIRS])


def inner(blocks, planes, s, hs, levels, columns_of, xs, inj):
    lane = lanes()
    tiles = range(1, 5)
    inside = (lane & 4) == 0
    for p in planes[0]:
        for f in range(5):
            own = None
            for tile in tiles:
                v = source(blocks, f, p, 8 * tile - 8, 8)
                s[p, f, 8 * tile : 8 * tile + 8, :] = v
                v = roll(v, tile * 8 + 4, 1)
                own = v if own is None else jnp.where(lane >= tile * 8, v, own)
            v, base = zcolumns(blocks, f, p)
            other = roll(v, 8 - base, 1)
            hs[p, f] = jnp.where(inside, other, own)
            xs[p, f] = jnp.where(inside, own, other)
    for p in planes[0]:
        for f in range(5):
            hs[p, f] = jnp.where(lane < 64, hs[p, f], roll(xs[p, f], 64, 1))
    for p in planes[0]:
        for q, v in enumerate(equilibrium(hs[p, 0], [hs[p, i] for i in (1, 2, 3)])):
            columns_of[0][p, q] = v
        for t in range(4):
            at = slice(8 + 8 * t, 16 + 8 * t)
            for q, v in enumerate(equilibrium(s[p, 0, at, :], [s[p, i, at, :] for i in (1, 2, 3)])):
                levels[0][p, q, at, :] = v
    for step in range(3):
        src, dst = levels[step], levels[step + 1]
        advance_columns(columns_of[step], columns_of[step + 1], hs, xs, inj, planes[step + 1], tiles)
        for p in planes[step + 1]:
            for t in range(4):
                at = slice(8 + 8 * t, 16 + 8 * t)
                for q, v in enumerate(collide(main_pull(src, inj, p, t), s[p, 4, at, :])):
                    dst[p, q, at, :] = v


def start_frame(s, g, p):
    parts = [framed(s, (p, i), 4) for i in range(4)]
    for q, v in enumerate(equilibrium(parts[0], parts[1:])):
        put_framed(g, (p, q), 4, v)


def advance_frame(src, dst, s, inj, p, radius):
    for q, v in enumerate(collide(frame_pull(src, inj, p, radius), framed(s, (p, 4), radius))):
        put_framed(dst, (p, q), radius, v)


OWN = [range(4, 8), range(5, 7), (), ()]
EARLY = [range(8, 10), range(7, 9), range(6, 8), ()]
LATE = [range(10, 12), range(9, 11), range(8, 10), range(7, 9)]
NEAR = [range(4, 12), range(5, 11), range(6, 10), range(7, 9)]
FAR = [range(0, 4), range(1, 5), range(2, 6), range(3, 7)]


def own_kernel(early, late, z, s, hs, g0, g1, g2, g3, h0, h1, h2, h3, xs, inj):
    inner((None, (early, late, z), None), OWN, s, hs, (g0, g1, g2, g3), (h0, h1, h2, h3), xs, inj)


def early_kernel(early, z, *refs):
    s, hs, g0, g1, g2, g3, h0, h1, h2, h3, xs, inj = refs[10:]
    inner((None, None, (early, None, z)), EARLY, s, hs, (g0, g1, g2, g3), (h0, h1, h2, h3), xs, inj)


def late_kernel(late, z, *refs):
    s, hs, g0, g1, g2, g3, h0, h1, h2, h3, xs, inj = refs[10:]
    inner((None, None, (None, late, z)), LATE, s, hs, (g0, g1, g2, g3), (h0, h1, h2, h3), xs, inj)


def far_kernel(early, late, *refs):
    s, hs, g0, g1, g2, g3, h0, h1, h2, h3, mid, xs, inj = refs[10:]
    inner(((early, late, late), None, None), FAR, s, hs, (g0, g1, g2, g3), (h0, h1, h2, h3), xs, inj)
    advance_columns(h3, None, hs, xs, inj, range(4, 8), range(1, 5))
    for p in range(4):
        for t in range(4):
            for i, v in enumerate(moments(main_pull(g3, inj, p + 4, t))):
                mid[i, p, 8 * t : 8 * t + 8, :] = v


def frames(halo, edge, planes, s, hs, levels, columns_of, ls, xs, inj):
    lane = lanes()
    inside = (lane & 4) == 0
    slot = lane & 56
    added = (slot == 0) | (slot == 40)
    for f in range(5):
        packed = edge(f)
        for p in planes[0]:
            v = halo(f, p)
            s[p, f, 4:8, :] = v[4:]
            s[p, f, 40:44, :] = v[:4]
            own = jnp.where(lane < 8, roll(v, 4, 1), roll(v, 44, 1))
            base = (p - planes[0][0]) * 8
            other = jnp.where(lane < 8, roll(packed, -base, 1), roll(packed, 40 - base, 1))
            ls[p, f] = jnp.where(inside, other, own)
            xs[p, f] = jnp.where(inside, own, other)
    for p in planes[0]:
        for f in range(5):
            v = jnp.where(lane < 64, ls[p, f], roll(xs[p, f], 64, 1))
            hs[p, f] = jnp.where(added, v, hs[p, f])
    for p in planes[0]:
        for q, v in enumerate(equilibrium(hs[p, 0], [hs[p, i] for i in (1, 2, 3)])):
            columns_of[0][p, q] = v
        start_frame(s, levels[0], p)
    for step in range(3):
        src, dst = levels[step], levels[step + 1]
        advance_columns(columns_of[step], columns_of[step + 1], hs, xs, inj, planes[step + 1], (0, 1, 4, 5))
        for p in planes[step + 1]:
            advance_frame(src, dst, s, inj, p, 3 - step)


def near_frame_kernel(from_core, from_chip, *refs):
    s, hs, g0, g1, g2, g3, h0, h1, h2, h3, ls, xs, inj = refs[10:]
    frames(
        lambda f, p: y_halo(from_core, from_chip, (f * 8 + p - 4) * 4),
        lambda f: y_halo(from_core, from_chip, 160 + f * 4),
        NEAR, s, hs, (g0, g1, g2, g3), (h0, h1, h2, h3), ls, xs, inj,
    )


def far_frame_kernel(halo, *refs):
    mid, density, momentum, s, hs, g0, g1, g2, g3, h0, h1, h2, h3, ls, xs, inj = refs[10:]
    frames(
        lambda f, p: halo[(f * 4 + p) * 8 : (f * 4 + p) * 8 + 8, :],
        lambda f: halo[160 + 8 * f : 168 + 8 * f, :],
        FAR, s, hs, (g0, g1, g2, g3), (h0, h1, h2, h3), ls, xs, inj,
    )
    advance_columns(h3, None, hs, xs, inj, range(4, 8), (1, 4))
    odd = lax.axis_index("gx") % 2
    sign = (1 - 2 * odd).astype(F32)
    for p in range(4):
        out = moments(frame_pull(g3, inj, p + 4, 0))
        plane = p + odd * (3 - 2 * p)
        for i in range(4):
            ref, index = (density, (plane,)) if i == 0 else (momentum, (i - 1, plane))
            scale = sign if i == 1 else 1.0
            ref[index] = mid[i, p] * scale
            ref[index + (slice(0, 4), slice(None))] = out[i][:4] * scale
            ref[index + (slice(28, 32), slice(None))] = out[i][4:] * scale


def call(kernel, out_shape, args, *, scratch=(), specs=None, limit=2 * MIB, flops=0, aliases=None):
    cost = pl.CostEstimate(flops=flops, bytes_accessed=0, transcendentals=0) if flops else None
    return pl.pallas_call(
        kernel,
        out_shape=out_shape,
        in_specs=specs or [VMEM] * len(args),
        out_specs=jax.tree.map(lambda _: VMEM, out_shape),
        scratch_shapes=scratch,
        input_output_aliases=aliases or {},
        cost_estimate=cost,
        compiler_params=pltpu.CompilerParams(vmem_limit_bytes=limit),
    )(*args)


def local(density, velocity, solid_mask):
    hbm = pl.BlockSpec(memory_space=pltpu.HBM)
    early, late, zcols = call(
        pack_kernel,
        (pltpu.VMEM((5, 2, 32, 128), F32), pltpu.VMEM((5, 2, 32, 128), F32), pltpu.VMEM((40, 128), F32)),
        (density, velocity, solid_mask),
        specs=[hbm] * 3,
        scratch=[
            pltpu.VMEM((4, 32, 128), F32),
            pltpu.VMEM((3, 4, 32, 128), F32),
            pltpu.VMEM((4, 32, 128), jnp.int32),
            pltpu.SemaphoreType.DMA((3,)),
        ],
        limit=PACK_LIMIT,
    )

    def pair(x, y, z):
        return x ^ 1, y, z

    def relay(x, y, z):
        return (x - 2 if x % 2 else x + 2), y, z

    early_pair = permuted(early, pair)
    zrecv = permuted(zcols, lambda x, y, z: (x, y, 1 - z))
    zdiag = permuted(zcols, lambda x, y, z: (x ^ 1, y, 1 - z))
    late_pair = permuted(late, pair)
    early_far = permuted(early_pair, relay)
    late_far = permuted(call(relay_message_kernel, pltpu.VMEM((360, 128), F32), (late_pair, zdiag)), relay)
    fields, level = pltpu.VMEM((12, 5, 48, 128), F32), pltpu.VMEM((12, 19, 48, 128), F32)
    column_fields, column_level = pltpu.VMEM((12, 5, 8, 128), F32), pltpu.VMEM((12, 19, 8, 128), F32)
    injected = pltpu.VMEM((12, 5, 48, 128), F32)
    state = (fields, column_fields) + (level,) * 4 + (column_level,) * 4
    work = [column_fields, injected]

    def stage(kernel, args, state_in, *, extra=(), before=(), scratch=work):
        count = len(args)
        return call(
            kernel,
            tuple(before) + state + tuple(extra),
            (*args, *state_in),
            scratch=scratch,
            limit=4 * MIB,
            flops=INNER_FLOPS,
            aliases={count + i: len(before) + i for i in range(len(state))} if state_in else None,
        )

    near = stage(own_kernel, (early, late, zrecv), ())
    to_core, to_chip = call(
        y_message_kernel,
        (pltpu.VMEM((184, 128), F32),) * 2,
        (early, late, zrecv, early_pair, late_pair, zdiag, near[1]),
    )
    from_core = permuted(to_core, lambda x, y, z: (x, y ^ 1, z))
    from_chip = permuted(to_chip, lambda x, y, z: (x, y + 1 if y % 2 else y - 1, z))
    near = stage(early_kernel, (early_pair, zdiag), near)
    near = stage(late_kernel, (late_pair, zdiag), near)
    halo_far = permuted(call(halo_message_kernel, pltpu.VMEM((200, 128), F32), (from_core, from_chip, near[1])), relay)
    near = stage(near_frame_kernel, (from_core, from_chip), near, scratch=[column_fields, *work])
    *far, mid = stage(far_kernel, (early_far, late_far), near, extra=[pltpu.VMEM((4, 4, 32, 128), F32)])
    outs = (jax.ShapeDtypeStruct((4, 32, 128), F32), jax.ShapeDtypeStruct((3, 4, 32, 128), F32))
    return tuple(
        call(
            far_frame_kernel,
            outs + state,
            (halo_far, *far, mid),
            scratch=[column_fields, *work],
            limit=4 * MIB,
            flops=INNER_FLOPS,
            aliases={1 + i: 2 + i for i in range(10)},
        )[:2]
    )


def solution(mesh):
    placed = (P("gx", "gy", "gz"), P(None, "gx", "gy", "gz"), P("gx", "gy", "gz"))
    return jax.shard_map(
        local,
        mesh=mesh,
        in_specs=placed,
        out_specs=(P("gx", "gy", "gz"), P(None, "gx", "gy", "gz")),
        check_vma=False,
    )
```

```python
import jax
import jax.numpy as jnp
from jax import lax
from jax.experimental import pallas as pl
from jax.experimental.pallas import tpu as pltpu
from jax.sharding import PartitionSpec as P


VELOCITIES = [
    (0, 0, 0),
    (1, 0, 0),
    (-1, 0, 0),
    (0, 1, 0),
    (0, -1, 0),
    (0, 0, 1),
    (0, 0, -1),
    (1, 1, 0),
    (-1, -1, 0),
    (1, -1, 0),
    (-1, 1, 0),
    (1, 0, 1),
    (-1, 0, -1),
    (1, 0, -1),
    (-1, 0, 1),
    (0, 1, 1),
    (0, -1, -1),
    (0, 1, -1),
    (0, -1, 1),
]
PAIRS = [(q, q + 1) for q in range(1, 19, 2)]
RELAX_RATE = 1.25
AXES = ("gx", "gy", "gz")
F32 = jnp.float32
VMEM = pl.BlockSpec(memory_space=pltpu.VMEM)
MIB = 1 << 20
CUT = 2
PACK_LIMIT = 66_500_000
INNER_FLOPS = 100_000_000


def lanes():
    return lax.broadcasted_iota(jnp.int32, (8, 128), 1)


def rows():
    return lax.broadcasted_iota(jnp.int32, (8, 128), 0)


def roll(v, shift, axis):
    shift %= v.shape[axis]
    return pltpu.roll(v, shift, axis) if shift else v


def permuted(x, target):
    pairs = []
    for gx in range(8):
        for gy in range(8):
            for gz in range(2):
                tx, ty, tz = target(gx, gy, gz)
                pairs.append(((gx * 8 + gy) * 2 + gz, ((tx % 8) * 8 + ty % 8) * 2 + tz % 2))
    return lax.ppermute(x, AXES, pairs)


def pack(odd, d, v, m, plane, at):
    src = plane + odd * (3 - 2 * plane)
    solid = m[src, at, :] == 1
    fields = [d[src, at, :]]
    fields += [jnp.where(solid, -v[i, src, at, :], v[i, src, at, :]) for i in range(3)]
    fields[1] = fields[1] * (1 - 2 * odd).astype(F32)
    fields.append(jnp.where(solid, 1.0, 0.0).astype(F32))
    return fields


def pack_early_kernel(d_hbm, v_hbm, m_hbm, early, d, v, m, sems):
    odd = lax.axis_index("gx") % 2
    copies = [
        pltpu.make_async_copy(src, dst, sems.at[i])
        for i, (src, dst) in enumerate(((v_hbm, v), (d_hbm, d), (m_hbm, m)))
    ]
    for copy in copies:
        copy.start()
    for copy in copies:
        copy.wait()
    for plane in range(CUT, 4):
        for t in range(4):
            at = pl.ds(8 * t, 8)
            for f, value in enumerate(pack(odd, d, v, m, plane, at)):
                early[f, plane - CUT, at, :] = value


def pack_late_kernel(d, v, m, late, zcols):
    odd = lax.axis_index("gx") % 2
    lane = lanes()
    packed = [jnp.zeros((8, 128), F32) for _ in range(5)]
    for plane in range(4):
        for t in range(4):
            at = pl.ds(8 * t, 8)
            base = plane * 32 + t * 8
            inside = (lane >= base) & (lane < base + 8)
            for f, value in enumerate(pack(odd, d, v, m, plane, at)):
                if plane < CUT:
                    late[f, plane, at, :] = value
                packed[f] = jnp.where(inside, roll(value, base + 4, 1), packed[f])
    for f in range(5):
        zcols[8 * f : 8 * f + 8, :] = packed[f]


def relay_message_kernel(late_pair, zdiag, out):
    for f in range(5):
        for plane in range(CUT):
            slab = (f * CUT + plane) * 32
            out[slab : slab + 32, :] = late_pair[f, plane]
    out[160 * CUT : 160 * CUT + 40, :] = zdiag[...]


def source(blocks, f, p, row, count):
    early, late, _ = blocks[p // 4]
    plane = (3 - p, p - 4, 11 - p)[p // 4]
    if plane >= CUT:
        v = early[f, plane - CUT, row : row + count, :]
    elif p >= 4:
        v = late[f, plane, row : row + count, :]
    else:
        slab = (f * CUT + plane) * 32
        v = late[slab + row : slab + row + count, :]
    return -v if f == 1 and not 4 <= p < 8 else v


def zcolumns(blocks, f, p):
    plane = (3 - p, p - 4, 11 - p)[p // 4]
    start = (160 * CUT if p < 4 else 0) + 8 * f
    v = blocks[p // 4][2][start : start + 8, :]
    return (-v if f == 1 and not 4 <= p < 8 else v), plane * 32


def y_message_kernel(early_own, late_own, zrecv, early_pair, late_pair, zdiag, _, to_core, to_chip):
    blocks = (None, (early_own, late_own, zrecv), (early_pair, late_pair, zdiag))
    first = lax.axis_index("gy") % 2 == 0
    lane = lanes()
    for f in range(5):
        for i in range(8):
            top = source(blocks, f, i + 4, 28, 4)
            bottom = source(blocks, f, i + 4, 0, 4)
            at = pl.ds((f * 8 + i) * 4, 4)
            to_core[at, :] = jnp.where(first, top, bottom)
            to_chip[at, :] = jnp.where(first, bottom, top)
        edge_low = jnp.zeros((8, 128), F32)
        edge_high = jnp.zeros((8, 128), F32)
        for i in range(8):
            z, base = zcolumns(blocks, f, i + 4)
            inside = (lane >= i * 8) & (lane < i * 8 + 8)
            edge_low = jnp.where(inside, roll(z, i * 8 - base, 1), edge_low)
            edge_high = jnp.where(inside, roll(z, i * 8 - base - 24, 1), edge_high)
        edge_high = roll(edge_high, 4, 0)
        at = pl.ds(160 + f * 4, 4)
        to_core[at, :] = jnp.where(first, edge_high, edge_low)[:4]
        to_chip[at, :] = jnp.where(first, edge_low, edge_high)[:4]


def y_halo(from_core, from_chip, row):
    first = lax.axis_index("gy") % 2 == 0
    a, b = from_core[row : row + 4, :], from_chip[row : row + 4, :]
    return jnp.concatenate([jnp.where(first, a, b), jnp.where(first, b, a)], axis=0)


def halo_message_kernel(from_core, from_chip, _, out):
    for f in range(5):
        for i in range(4):
            at = (f * 4 + i) * 8
            out[at : at + 8, :] = y_halo(from_core, from_chip, (f * 8 + 4 + i) * 4)
        out[160 + 8 * f : 168 + 8 * f, :] = roll(y_halo(from_core, from_chip, 160 + f * 4), -32, 1)


def populations(weighted, base, h, rest):
    even, odd = [], []
    double = weighted + weighted
    base2 = base + base
    for q, _ in PAIRS:
        c = VELOCITIES[q]
        terms = [(h[i], c[i]) for i in range(3) if c[i]]
        k = terms[0][0]
        if len(terms) == 2:
            k = k + terms[1][0] if terms[1][1] > 0 else k - terms[1][0]
            m = weighted * k
            even.append(base + m * k)
        else:
            m = double * k
            even.append(base2 + m * k)
        odd.append(m)
    return rest * base, even, odd


def equilibrium(density, velocity):
    h = [1.5 * u for u in velocity]
    w = density * (1.0 / 36.0)
    square = h[0] * h[0] + h[1] * h[1] + h[2] * h[2]
    still, even, odd = populations(w + w, w - w * (square * (2.0 / 3.0)), h, 12.0)
    out = [still]
    for e, o in zip(even, odd):
        out += [e + o, e - o]
    return out


def momentum_of(diff):
    total = [None, None, None]
    for (q, _), d in zip(PAIRS, diff):
        for i in range(3):
            c = VELOCITIES[q][i]
            if c:
                total[i] = d if total[i] is None else total[i] + d if c > 0 else total[i] - d
    return total


def collide(f, mask):
    total = [f[a] + f[b] for a, b in PAIRS]
    diff = [f[a] - f[b] for a, b in PAIRS]
    r = f[0]
    for s in total:
        r = r + s
    j = momentum_of(diff)
    solid = mask > 0.5
    inverse = jnp.where(solid, 0.0, 1.5 / r)
    w = jnp.where(solid, 0.0, r * (RELAX_RATE / 36.0))
    h = [x * inverse for x in j]
    square = h[0] * h[0] + h[1] * h[1] + h[2] * h[2]
    still, even, odd = populations(w + w, w - w * (square * (2.0 / 3.0)), h, 12.0)
    a = jnp.where(solid, 0.5, 0.5 * (1.0 - RELAX_RATE))
    b = jnp.where(solid, -0.5, 0.5 * (1.0 - RELAX_RATE))
    out = [still + (a + a) * f[0]]
    for s, d, e, o in zip(total, diff, even, odd):
        p, m = a * s + e, b * d + o
        out += [p + m, p - m]
    return out


PLUS = [5, 11, 14, 15, 18]
MINUS = [6, 12, 13, 16, 17]


def streamed_column(hg, q, p, turn=0):
    cx, cy, cz = VELOCITIES[q]
    v = hg[p - cx, q]
    if not cy:
        return roll(v, cz + turn, 1)
    v = roll(v, cy, 0)
    edge = 0 if cy > 0 else 7
    return jnp.where(rows() == edge, roll(v, cz + turn + 8 * cy, 1), roll(v, cz + turn, 1))


def advance_columns(src, dst, hs, xs, inj, planes, tiles):
    inner = (lanes() & 7) >= 4
    for p in planes:
        f = [streamed_column(src, q, p) if dst is not None or q in PLUS else None for q in range(19)]
        for k in range(5):
            xs[p, k] = jnp.where(inner, f[PLUS[k]], streamed_column(src, MINUS[k], p, 64))
        if dst is not None:
            for q, v in enumerate(collide(f, hs[p, 4])):
                dst[p, q] = v
    for p in planes:
        for k in range(5):
            x = xs[p, k]
            for tile in tiles:
                inj[p, k, 8 * tile : 8 * tile + 8, :] = roll(x, -(tile * 8 + 4), 1)


def pulled(load, edge):
    lane = lanes()
    sides = [edge(k) for k in range(5)]
    out = []
    for q in range(19):
        cz = VELOCITIES[q][2]
        v = load(q)
        if cz > 0:
            v = jnp.where(lane == 0, sides[PLUS.index(q)], roll(v, 1, 1))
        elif cz < 0:
            v = jnp.where(lane == 127, sides[MINUS.index(q)], roll(v, 127, 1))
        out.append(v)
    return out


def main_pull(g, inj, p, t):
    def load(q):
        cx, cy, _ = VELOCITIES[q]
        return g[p - cx, q, 8 + 8 * t - cy : 16 + 8 * t - cy, :]

    return pulled(load, lambda k: inj[p, k, 8 + 8 * t : 16 + 8 * t, :])


def framed(ref, index, radius, shift=0):
    top = ref[index + (slice(8 - radius - shift, 16 - radius - shift), slice(None))]
    bottom = ref[index + (slice(32 + radius - shift, 40 + radius - shift), slice(None))]
    return jnp.where(rows() < 4, top, bottom)


def put_framed(ref, index, radius, v):
    ref[index + (slice(8 - radius, 12 - radius), slice(None))] = v[:4]
    ref[index + (slice(36 + radius, 40 + radius), slice(None))] = v[4:]


def frame_pull(g, inj, p, radius):
    def load(q):
        cx, cy, _ = VELOCITIES[q]
        return framed(g, (p - cx, q), radius, cy)

    return pulled(load, lambda k: framed(inj, (p, k), radius))


def moments(f):
    r = f[0]
    for a, b in PAIRS:
        r = r + (f[a] + f[b])
    return [r] + momentum_of([f[a] - f[b] for a, b in PAIRS])


def inner(blocks, planes, s, hs, levels, columns_of, xs, inj):
    lane = lanes()
    tiles = range(1, 5)
    inside = (lane & 4) == 0
    for p in planes[0]:
        for f in range(5):
            own = None
            for tile in tiles:
                v = source(blocks, f, p, 8 * tile - 8, 8)
                s[p, f, 8 * tile : 8 * tile + 8, :] = v
                v = roll(v, tile * 8 + 4, 1)
                own = v if own is None else jnp.where(lane >= tile * 8, v, own)
            v, base = zcolumns(blocks, f, p)
            other = roll(v, 8 - base, 1)
            hs[p, f] = jnp.where(inside, other, own)
            xs[p, f] = jnp.where(inside, own, other)
    for p in planes[0]:
        for f in range(5):
            hs[p, f] = jnp.where(lane < 64, hs[p, f], roll(xs[p, f], 64, 1))
    for p in planes[0]:
        for q, v in enumerate(equilibrium(hs[p, 0], [hs[p, i] for i in (1, 2, 3)])):
            columns_of[0][p, q] = v
        for t in range(4):
            at = slice(8 + 8 * t, 16 + 8 * t)
            for q, v in enumerate(equilibrium(s[p, 0, at, :], [s[p, i, at, :] for i in (1, 2, 3)])):
                levels[0][p, q, at, :] = v
    for step in range(3):
        src, dst = levels[step], levels[step + 1]
        advance_columns(columns_of[step], columns_of[step + 1], hs, xs, inj, planes[step + 1], tiles)
        for p in planes[step + 1]:
            for t in range(4):
                at = slice(8 + 8 * t, 16 + 8 * t)
                for q, v in enumerate(collide(main_pull(src, inj, p, t), s[p, 4, at, :])):
                    dst[p, q, at, :] = v


def start_frame(s, g, p):
    parts = [framed(s, (p, i), 4) for i in range(4)]
    for q, v in enumerate(equilibrium(parts[0], parts[1:])):
        put_framed(g, (p, q), 4, v)


def advance_frame(src, dst, s, inj, p, radius):
    for q, v in enumerate(collide(frame_pull(src, inj, p, radius), framed(s, (p, 4), radius))):
        put_framed(dst, (p, q), radius, v)


OWN = [range(4, 8), range(5, 7), (), ()]
KNOWN = 12 - CUT
EARLY = [range(8, KNOWN), range(7, KNOWN - 1), range(6, KNOWN - 2), range(7, KNOWN - 3)]
LATE = [range(KNOWN, 12), range(KNOWN - 1, 11), range(KNOWN - 2, 10), range(max(KNOWN - 3, 7), 9)]
NEAR = [range(4, 12), range(5, 11), range(6, 10), range(7, 9)]
FAR = [range(0, 4), range(1, 5), range(2, 6), range(3, 7)]


def own_kernel(early, late, z, s, hs, g0, g1, g2, g3, h0, h1, h2, h3, xs, inj):
    inner((None, (early, late, z), None), OWN, s, hs, (g0, g1, g2, g3), (h0, h1, h2, h3), xs, inj)


def early_kernel(early, z, *refs):
    s, hs, g0, g1, g2, g3, h0, h1, h2, h3, xs, inj = refs[10:]
    inner((None, None, (early, None, z)), EARLY, s, hs, (g0, g1, g2, g3), (h0, h1, h2, h3), xs, inj)


def late_kernel(late, z, *refs):
    s, hs, g0, g1, g2, g3, h0, h1, h2, h3, xs, inj = refs[10:]
    inner((None, None, (None, late, z)), LATE, s, hs, (g0, g1, g2, g3), (h0, h1, h2, h3), xs, inj)


def far_kernel(early, late, *refs):
    s, hs, g0, g1, g2, g3, h0, h1, h2, h3, mid, xs, inj = refs[10:]
    inner(((early, late, late), None, None), FAR, s, hs, (g0, g1, g2, g3), (h0, h1, h2, h3), xs, inj)
    advance_columns(h3, None, hs, xs, inj, range(4, 8), range(1, 5))
    for p in range(4):
        for t in range(4):
            for i, v in enumerate(moments(main_pull(g3, inj, p + 4, t))):
                mid[i, p, 8 * t : 8 * t + 8, :] = v


def frames(halo, edge, planes, s, hs, levels, columns_of, ls, xs, inj):
    lane = lanes()
    inside = (lane & 4) == 0
    slot = lane & 56
    added = (slot == 0) | (slot == 40)
    for f in range(5):
        packed = edge(f)
        for p in planes[0]:
            v = halo(f, p)
            s[p, f, 4:8, :] = v[4:]
            s[p, f, 40:44, :] = v[:4]
            own = jnp.where(lane < 8, roll(v, 4, 1), roll(v, 44, 1))
            base = (p - planes[0][0]) * 8
            other = jnp.where(lane < 8, roll(packed, -base, 1), roll(packed, 40 - base, 1))
            ls[p, f] = jnp.where(inside, other, own)
            xs[p, f] = jnp.where(inside, own, other)
    for p in planes[0]:
        for f in range(5):
            v = jnp.where(lane < 64, ls[p, f], roll(xs[p, f], 64, 1))
            hs[p, f] = jnp.where(added, v, hs[p, f])
    for p in planes[0]:
        for q, v in enumerate(equilibrium(hs[p, 0], [hs[p, i] for i in (1, 2, 3)])):
            columns_of[0][p, q] = v
        start_frame(s, levels[0], p)
    for step in range(3):
        src, dst = levels[step], levels[step + 1]
        advance_columns(columns_of[step], columns_of[step + 1], hs, xs, inj, planes[step + 1], (0, 1, 4, 5))
        for p in planes[step + 1]:
            advance_frame(src, dst, s, inj, p, 3 - step)


def near_frame_kernel(from_core, from_chip, *refs):
    s, hs, g0, g1, g2, g3, h0, h1, h2, h3, ls, xs, inj = refs[10:]
    frames(
        lambda f, p: y_halo(from_core, from_chip, (f * 8 + p - 4) * 4),
        lambda f: y_halo(from_core, from_chip, 160 + f * 4),
        NEAR, s, hs, (g0, g1, g2, g3), (h0, h1, h2, h3), ls, xs, inj,
    )


def far_frame_kernel(halo, *refs):
    mid, density, momentum, s, hs, g0, g1, g2, g3, h0, h1, h2, h3, ls, xs, inj = refs[10:]
    frames(
        lambda f, p: halo[(f * 4 + p) * 8 : (f * 4 + p) * 8 + 8, :],
        lambda f: halo[160 + 8 * f : 168 + 8 * f, :],
        FAR, s, hs, (g0, g1, g2, g3), (h0, h1, h2, h3), ls, xs, inj,
    )
    advance_columns(h3, None, hs, xs, inj, range(4, 8), (1, 4))
    odd = lax.axis_index("gx") % 2
    sign = (1 - 2 * odd).astype(F32)
    for p in range(4):
        out = moments(frame_pull(g3, inj, p + 4, 0))
        plane = p + odd * (3 - 2 * p)
        for i in range(4):
            ref, index = (density, (plane,)) if i == 0 else (momentum, (i - 1, plane))
            scale = sign if i == 1 else 1.0
            ref[index] = mid[i, p] * scale
            ref[index + (slice(0, 4), slice(None))] = out[i][:4] * scale
            ref[index + (slice(28, 32), slice(None))] = out[i][4:] * scale


def call(kernel, out_shape, args, *, scratch=(), specs=None, limit=2 * MIB, flops=0, aliases=None):
    cost = pl.CostEstimate(flops=flops, bytes_accessed=0, transcendentals=0) if flops else None
    return pl.pallas_call(
        kernel,
        out_shape=out_shape,
        in_specs=specs or [VMEM] * len(args),
        out_specs=jax.tree.map(lambda _: VMEM, out_shape),
        scratch_shapes=scratch,
        input_output_aliases=aliases or {},
        cost_estimate=cost,
        compiler_params=pltpu.CompilerParams(vmem_limit_bytes=limit),
    )(*args)


def local(density, velocity, solid_mask):
    hbm = pl.BlockSpec(memory_space=pltpu.HBM)
    block = pltpu.VMEM((4, 32, 128), F32), pltpu.VMEM((3, 4, 32, 128), F32), pltpu.VMEM((4, 32, 128), jnp.int32)
    early, *raw = call(
        pack_early_kernel,
        (pltpu.VMEM((5, 4 - CUT, 32, 128), F32), *block),
        (density, velocity, solid_mask),
        specs=[hbm] * 3,
        scratch=[pltpu.SemaphoreType.DMA((3,))],
        limit=PACK_LIMIT,
    )
    late, zcols = call(pack_late_kernel, (pltpu.VMEM((5, CUT, 32, 128), F32), pltpu.VMEM((40, 128), F32)), raw)

    def pair(x, y, z):
        return x ^ 1, y, z

    def relay(x, y, z):
        return (x - 2 if x % 2 else x + 2), y, z

    early_pair = permuted(early, pair)
    zrecv = permuted(zcols, lambda x, y, z: (x, y, 1 - z))
    zdiag = permuted(zcols, lambda x, y, z: (x ^ 1, y, 1 - z))
    late_pair = permuted(late, pair)
    early_far = permuted(early_pair, relay)
    late_far = permuted(call(relay_message_kernel, pltpu.VMEM((160 * CUT + 40, 128), F32), (late_pair, zdiag)), relay)
    fields, level = pltpu.VMEM((12, 5, 48, 128), F32), pltpu.VMEM((12, 19, 48, 128), F32)
    column_fields, column_level = pltpu.VMEM((12, 5, 8, 128), F32), pltpu.VMEM((12, 19, 8, 128), F32)
    injected = pltpu.VMEM((12, 5, 48, 128), F32)
    state = (fields, column_fields) + (level,) * 4 + (column_level,) * 4
    work = [column_fields, injected]

    def stage(kernel, args, state_in, *, extra=(), before=(), scratch=work):
        count = len(args)
        return call(
            kernel,
            tuple(before) + state + tuple(extra),
            (*args, *state_in),
            scratch=scratch,
            limit=4 * MIB,
            flops=INNER_FLOPS,
            aliases={count + i: len(before) + i for i in range(len(state))} if state_in else None,
        )

    near = stage(own_kernel, (early, late, zrecv), ())
    to_core, to_chip = call(
        y_message_kernel,
        (pltpu.VMEM((184, 128), F32),) * 2,
        (early, late, zrecv, early_pair, late_pair, zdiag, near[1]),
    )
    from_core = permuted(to_core, lambda x, y, z: (x, y ^ 1, z))
    from_chip = permuted(to_chip, lambda x, y, z: (x, y + 1 if y % 2 else y - 1, z))
    near = stage(early_kernel, (early_pair, zdiag), near)
    near = stage(late_kernel, (late_pair, zdiag), near)
    halo_far = permuted(call(halo_message_kernel, pltpu.VMEM((200, 128), F32), (from_core, from_chip, near[1])), relay)
    near = stage(near_frame_kernel, (from_core, from_chip), near, scratch=[column_fields, *work])
    *far, mid = stage(far_kernel, (early_far, late_far), near, extra=[pltpu.VMEM((4, 4, 32, 128), F32)])
    outs = (jax.ShapeDtypeStruct((4, 32, 128), F32), jax.ShapeDtypeStruct((3, 4, 32, 128), F32))
    return tuple(
        call(
            far_frame_kernel,
            outs + state,
            (halo_far, *far, mid),
            scratch=[column_fields, *work],
            limit=4 * MIB,
            flops=INNER_FLOPS,
            aliases={1 + i: 2 + i for i in range(10)},
        )[:2]
    )


def solution(mesh):
    placed = (P("gx", "gy", "gz"), P(None, "gx", "gy", "gz"), P("gx", "gy", "gz"))
    return jax.shard_map(
        local,
        mesh=mesh,
        in_specs=placed,
        out_specs=(P("gx", "gy", "gz"), P(None, "gx", "gy", "gz")),
        check_vma=False,
    )
```
